128 devices in a mesh: data: 1, dap: 128 (over z, y, x, core).
Axes of the slice: x: 4, y: 4, z: 4, core: 2. Of those that a mesh axis runs over, the one named last changes fastest.
Arguments:
- z: bfloat16 [1024, 1024, 64], P(('data', 'dap'))
- res_mask: int32 [1024], P('data')
- ln_w: bfloat16 [3, 2, 2, 64], replicated
- w_in: bfloat16 [3, 2, 64, 256], replicated
- b_g: bfloat16 [3, 2, 64], replicated
- w_b: bfloat16 [3, 2, 64, 4], replicated
- w_o: bfloat16 [3, 2, 64, 64], replicated
- b_o: bfloat16 [3, 2, 64], replicated
Outputs:
- output: bfloat16 [1024, 1024, 64], P(('data', 'dap'))
All inputs are finite; a program needn't handle non-finite values.
Results may differ from the reference program's by a relative error of at most 0.0117227.
Values are sent between devices in bfloat16 or wider.
A program may use at most 1 GiB of HBM per device.

```python
import jax
import jax.numpy as jnp
from jax import lax

NR = 1024
C_Z = 64
HEADS = 4
HEAD = 16
LAYERS = 3

EPS = 1e-5
NEG = -1e9


def setup_inputs(seed: int = 0, part: int = 0) -> dict:
    key = jax.random.PRNGKey(seed)
    kz, km = jax.random.split(jax.random.fold_in(jax.random.fold_in(key, 1), part))
    kw = jax.random.split(jax.random.fold_in(key, 0), 7)
    hd = HEADS * HEAD
    z = jax.random.normal(kz, (NR, NR, C_Z), jnp.float32)
    keep = jax.random.uniform(km, (NR,), jnp.float32) > 0.2
    res_mask = jnp.where(jnp.arange(NR) == 0, True, keep).astype(jnp.int32)
    gamma = 1.0 + 0.1 * jax.random.normal(kw[0], (LAYERS, 2, 1, C_Z), jnp.float32)
    beta = 0.1 * jax.random.normal(kw[1], (LAYERS, 2, 1, C_Z), jnp.float32)
    w_in = jax.random.normal(kw[2], (LAYERS, 2, C_Z, 4 * hd), jnp.float32) * C_Z ** -0.5
    b_g = 0.5 * jax.random.normal(kw[3], (LAYERS, 2, hd), jnp.float32)
    w_b = 1.5 * jax.random.normal(kw[4], (LAYERS, 2, C_Z, HEADS), jnp.float32) * C_Z ** -0.5
    w_o = jax.random.normal(kw[5], (LAYERS, 2, hd, C_Z), jnp.float32) * hd ** -0.5
    b_o = 0.1 * jax.random.normal(kw[6], (LAYERS, 2, C_Z), jnp.float32)
    bf = jnp.bfloat16
    return {'z': z.astype(bf), 'res_mask': res_mask,
            'ln_w': jnp.concatenate([gamma, beta], axis=2).astype(bf),
            'w_in': w_in.astype(bf), 'b_g': b_g.astype(bf), 'w_b': w_b.astype(bf),
            'w_o': w_o.astype(bf), 'b_o': b_o.astype(bf)}


def _ln(x, w):
    x = x.astype(jnp.float32)
    mu = jnp.mean(x, axis=-1, keepdims=True)
    var = jnp.mean(jnp.square(x - mu), axis=-1, keepdims=True)
    y = (x - mu) * lax.rsqrt(var + EPS)
    return (y * w[0].astype(jnp.float32) + w[1].astype(jnp.float32)).astype(jnp.bfloat16)


def _tri_start(z, res_mask, ln_w, w_in, b_g, w_b, w_o, b_o):
    def pair_bias(zr):
        return jnp.dot(_ln(zr, ln_w), w_b, preferred_element_type=jnp.float32).astype(jnp.bfloat16)
    b = lax.map(pair_bias, z)
    mask_bias = jnp.where(res_mask > 0, 0.0, NEG)
    bias = jnp.transpose(b, (2, 0, 1)).astype(jnp.float32) + mask_bias[None, None, :]
    gate_b = b_g.astype(jnp.float32).reshape(HEADS, HEAD)

    def row(zr):
        y = _ln(zr, ln_w)
        proj = jnp.dot(y, w_in, preferred_element_type=jnp.float32).reshape(NR, 4, HEADS, HEAD)
        q = proj[:, 0].astype(jnp.bfloat16)
        k = proj[:, 1].astype(jnp.bfloat16)
        v = proj[:, 2].astype(jnp.bfloat16)
        g = jax.nn.sigmoid(proj[:, 3] + gate_b)
        s = jnp.einsum('jhd,khd->hjk', q.astype(jnp.float32), k.astype(jnp.float32)) * HEAD ** -0.5 + bias
        p = jax.nn.softmax(s, axis=-1).astype(jnp.bfloat16)
        o = jnp.einsum('hjk,khd->jhd', p.astype(jnp.float32), v.astype(jnp.float32))
        o = (g * o).astype(jnp.bfloat16).reshape(NR, HEADS * HEAD)
        upd = jnp.dot(o, w_o, preferred_element_type=jnp.float32) + b_o.astype(jnp.float32)
        return (zr.astype(jnp.float32) + upd).astype(jnp.bfloat16)

    return lax.map(row, z)


def reference(z, res_mask, ln_w, w_in, b_g, w_b, w_o, b_o):
    def layer(z, w):
        lw, wi, bg, wb, wo, bo = w
        z = _tri_start(z, res_mask, lw[0], wi[0], bg[0], wb[0], wo[0], bo[0])
        zt = _tri_start(jnp.swapaxes(z, 0, 1), res_mask, lw[1], wi[1], bg[1], wb[1], wo[1], bo[1])
        return jnp.swapaxes(zt, 0, 1), None
    z, _ = lax.scan(layer, z, (ln_w, w_in, b_g, w_b, w_o, b_o))
    return z
```

```python
import functools, math
import jax, jax.numpy as jnp
from jax import lax
from jax.experimental import pallas as pl
from jax.experimental.pallas import tpu as pltpu
from jax.sharding import PartitionSpec as P
F32=jnp.float32; BF16=jnp.bfloat16
EPS=1e-5; NEG=-1e9
LOG2E=1.4426950408889634
MX=256

def _ln_t(x, gamma, beta):
    mu = jnp.mean(x, axis=0, keepdims=True)
    d = x - mu
    var = jnp.mean(d*d, axis=0, keepdims=True)
    return (d * lax.rsqrt(var + EPS) * gamma + beta).astype(BF16)

def fast_kernel(R, N, C, H, LAG, NR, OA, FD,
               z_ref, bias_ref, mask_ref, lnw_ref, wqvt_ref, wk2_ref, bg_ref, wo_ref, bo_ref, lnn_ref, wbn_ref,
               out_ref, bnext_ref,
               k_s, q_s, v_s, g_s, o_s, y_s, bias_s):
    jb = pl.program_id(0)
    D = C // H
    QB = MX
    KC = 128
    CH = N // KC
    q0 = pl.multiple_of(jb * QB, QB)

    def body(*accs):
        sacc = [accs[0:NR], accs[NR:2*NR]]
        oacc = [accs[2*NR:2*NR+OA], accs[2*NR+OA:2*NR+2*OA]]
        z128 = jnp.zeros((KC, MX-KC), BF16)
        zrow = lambda n: jnp.zeros((n, MX), BF16)

        @pl.when(jb == 0)
        def _():
            def prep(i, _):
                y = _ln_t(z_ref[i].astype(F32), lnw_ref[:, 0:1], lnw_ref[:, 1:2])
                yt = jnp.concatenate([y, jnp.zeros((KC-C, N), BF16)], axis=0).T
                for j in range(N//MX):
                    m = j % 2
                    cs = slice(j*MX, (j+1)*MX)
                    pltpu.matmul_push_rhs(jnp.concatenate([y[:, cs], zrow(MX-C)], axis=0), staging_register=0, mxu_index=m)
                    pltpu.matmul_acc_lhs(sacc[m][0], wqvt_ref[0:KC], load_staged_rhs=0)
                    pltpu.matmul_acc_lhs(sacc[m][1], wqvt_ref[KC:2*KC])
                    pltpu.matmul_push_rhs(wk2_ref[...], staging_register=1, mxu_index=m)
                    for r in range(2):
                        kk = jnp.concatenate([yt[j*MX+r*KC:j*MX+(r+1)*KC], z128], axis=1)
                        pltpu.matmul_acc_lhs(sacc[m][2+r], kk, load_staged_rhs=1 if r == 0 else None)
                    qv = pltpu.matmul_pop(sacc[m][0])
                    q = qv[0:C].astype(BF16).astype(F32) * (LOG2E * D ** -0.5)
                    qh = q.astype(BF16)
                    ql = (q - qh.astype(F32)).astype(BF16)
                    for h in range(H):
                        q_s[i, 2*D*h:2*D*h+D, cs] = qh[D*h:D*h+D]
                        q_s[i, 2*D*h+D:2*D*h+2*D, cs] = ql[D*h:D*h+D]
                    v_s[i, :, cs] = qv[C:2*C].astype(BF16)
                    t = pltpu.matmul_pop(sacc[m][1])
                    g_s[i, :, cs] = jax.nn.sigmoid(t[0:C] + bg_ref[...])
                    for r in range(2):
                        k_s[i, j*MX+r*KC:j*MX+(r+1)*KC] = pltpu.matmul_pop(sacc[m][2+r])[:, 0:2*C].astype(BF16)
                return 0
            lax.fori_loop(0, R, prep, 0)

        for h in range(H):
            for c in range(CH):
                sl = slice(c*KC, (c+1)*KC)
                for w in range(2):
                    bias_s[h, sl, w*128:(w+1)*128] = bias_ref[h, sl, w*128:(w+1)*128].astype(F32) * LOG2E + mask_ref[sl]

        zp = jnp.zeros((KC, QB), BF16)
        zv = jnp.zeros((2*D, MX-KC), BF16)
        zq = jnp.zeros((2*D, QB), BF16)
        ones = jnp.where(lax.broadcasted_iota(jnp.int32, (D, KC), 0) == 0, 1.0, 0.0).astype(BF16)
        steps = [(h, c) for h in range(H) for c in range(CH)]
        S = len(steps)

        def pair(t, _):
            es = {}
            def tile(n):
                for m in range(2):
                    p = es.pop((n, m)) if n >= 0 else zp
                    if n+LAG < S:
                        h, c = steps[n+LAG]
                        w = jnp.concatenate([zq]*h + [q_s[2*t+m, 2*D*h:2*D*(h+1), pl.ds(q0, QB)]] + [zq]*(H-1-h), axis=0)
                    else:
                        w = zp
                    pltpu.matmul_push_rhs(jnp.concatenate([p, w], axis=0), staging_register=n % 2, mxu_index=m)
            def accum(n):
                for m in range(2):
                    ld = n % 2
                    if n+LAG < S:
                        h, c = steps[n+LAG]
                        kk = jnp.concatenate([z128, k_s[2*t+m, c*KC:(c+1)*KC]], axis=1)
                        pltpu.matmul_acc_lhs(sacc[m][(n+LAG) % NR], kk, load_staged_rhs=ld)
                        ld = None
                    if n >= 0:
                        h, c = steps[n]
                        vv = jnp.concatenate([v_s[2*t+m, D*h:D*h+D, c*KC:(c+1)*KC], ones], axis=0)
                        pltpu.matmul_acc_lhs(oacc[m][h % OA], jnp.concatenate([vv, zv], axis=1), load_staged_rhs=ld)
            def ex(n):
                h, c = steps[n]
                b = bias_s[h, c*KC:(c+1)*KC]
                for m in range(2):
                    es[n, m] = jnp.exp2(pltpu.matmul_pop(sacc[m][n % NR]) + b).astype(BF16)
            def fin(n):
                h, c = steps[n]
                if c == CH-1:
                    for m in range(2):
                        i = 2*t+m
                        a = pltpu.matmul_pop(oacc[m][h % OA])
                        o_s[i, D*h:D*h+D] = (g_s[i, D*h:D*h+D, pl.ds(q0, QB)] * (a[0:D] / a[D:D+1])).astype(BF16)
            for n in range(-LAG, S):
                if n >= 0: ex(n)
                tile(n); accum(n)
                if n-FD >= 0: fin(n-FD)
            for n in range(S-FD, S): fin(n)
            return 0
        lax.fori_loop(0, R//2, pair, 0)

        def upd(t, _):
            for m in range(2):
                pltpu.matmul_push_rhs(jnp.concatenate([o_s[2*t+m], zrow(MX-C)], axis=0), staging_register=0, mxu_index=m)
                pltpu.matmul_acc_lhs(sacc[m][0], wo_ref[...], load_staged_rhs=0)
            for m in range(2):
                i = 2*t+m
                u = pltpu.matmul_pop(sacc[m][0])[0:C] + bo_ref[...]
                zn = (z_ref[i, :, pl.ds(q0, QB)].astype(F32) + u).astype(BF16)
                out_ref[i] = zn
                y_s[pl.ds(pl.multiple_of(i*C, C), C)] = _ln_t(zn.astype(F32), lnn_ref[:, 0:1], lnn_ref[:, 1:2])
            return 0
        lax.fori_loop(0, R//2, upd, 0)
        for m in range(2):
            pltpu.matmul_push_rhs(y_s[m*MX:(m+1)*MX], staging_register=0, mxu_index=m)
            pltpu.matmul_acc_lhs(oacc[m][0], wbn_ref[:, m*MX:(m+1)*MX], load_staged_rhs=0)
        bnext_ref[...] = (pltpu.matmul_pop(oacc[0][0]) + pltpu.matmul_pop(oacc[1][0])).astype(BF16)

    pl.run_scoped(body, *[pltpu.ACC(m)((KC, MX), F32) for m in range(2) for _ in range(NR)],
                  *[pltpu.ACC(m)((2*D, MX), F32) for m in range(2) for _ in range(OA)])

def attention(z, bias, mask, lnw, wqvt, wk2, bg, wo, bo, lnn, wbn, LAG=4, NR=5, OA=2, FD=3, FL={}):
    R, C, N = z.shape
    H = bias.shape[0]
    QB = MX
    full = lambda a: pl.BlockSpec(a.shape, lambda j: (0,)*a.ndim, pipeline_mode=pl.Buffered(1))
    return pl.pallas_call(
        functools.partial(fast_kernel, R, N, C, H, LAG, NR, OA, FD),
        grid=(N//QB,),
        in_specs=[full(z), pl.BlockSpec((H, N, QB), lambda j: (0, 0, j)), full(mask), full(lnw), full(wqvt), full(wk2),
                  full(bg), full(wo), full(bo), full(lnn), full(wbn)],
        out_specs=[pl.BlockSpec((R, C, QB), lambda j: (0, 0, j)), pl.BlockSpec((H*R, QB), lambda j: (0, j))],
        out_shape=[jax.ShapeDtypeStruct((R, C, N), BF16), jax.ShapeDtypeStruct((H*R, N), BF16)],
        scratch_shapes=[pltpu.VMEM((R, N, 2*C), BF16), pltpu.VMEM((R, 2*C, N), BF16), pltpu.VMEM((R, C, N), BF16),
                        pltpu.VMEM((R, C, N), F32), pltpu.VMEM((R, C, QB), BF16), pltpu.VMEM((R*C, QB), BF16),
                        pltpu.VMEM((H, N, QB), F32)],
        compiler_params=pltpu.CompilerParams(dimension_semantics=("arbitrary",), vmem_limit_bytes=48*2**20, flags=FL),
        name="att_fast",
    )(z, bias, mask, lnw, wqvt, wk2, bg, wo, bo, lnn, wbn)

def prep_weights(ln_w, w_in, b_g, w_b, w_o, b_o, R):
    C = w_o.shape[0]; H = w_b.shape[1]; D = C // H
    lnw = ln_w.astype(F32).T
    wq, wk, wv, wt = (w_in[:, i*C:(i+1)*C] for i in range(4))
    wqvt = jnp.pad(jnp.concatenate([wq, wv, wt], axis=1).T, ((0, MX-3*C), (0, MX-C)))
    wk2 = jnp.concatenate([wk.reshape(C, H, 1, D)]*2, axis=2).reshape(C, 2*C)
    wk2 = jnp.pad(wk2, ((0, MX-C), (0, MX-2*C)))
    bg = b_g.astype(F32).reshape(C, 1)
    bo = b_o.astype(F32).reshape(C, 1)
    eye = jnp.eye(R, dtype=w_b.dtype)
    wbn = (w_b.T[:, None, None, :] * eye[None, :, :, None]).reshape(H*R, R*C)
    wo = jnp.pad(w_o.T, ((0, 2*C-C), (0, MX-C)))
    return lnw, wqvt, wk2, bg, wo, bo, wbn


def safe_kernel(R, N, C, H, QB, KC,
               z_ref, bias_ref, mask_ref, lnw_ref, wqvt_ref, wk2_ref, bg_ref, wo_ref, bo_ref, lnn_ref, wbn_ref,
               out_ref, bnext_ref,
               k_s, q_s, v_s, g_s, o_s, y_s, bias_s, s_s):
    jb = pl.program_id(0)
    D = C // H

    @pl.when(jb == 0)
    def _():
        rows = lax.broadcasted_iota(jnp.int32, (16, N), 0)
        ones = jnp.where(rows == 0, 1.0, 0.0).astype(BF16)
        def prep(i, _):
            x = z_ref[i].astype(F32)
            y = _ln_t(x, lnw_ref[:, 0:1], lnw_ref[:, 1:2])
            p = jnp.dot(wqvt_ref[0:3*C, 0:C], y, preferred_element_type=F32)
            yt = y.T
            k2 = jnp.dot(yt, wk2_ref[0:C, 0:2*C], preferred_element_type=F32).astype(BF16)
            k_s[i] = k2
            q = p[0:C].astype(BF16).astype(F32) * (LOG2E * D ** -0.5)
            qh = q.astype(BF16)
            ql = (q - qh.astype(F32)).astype(BF16)
            v = p[C:2*C].astype(BF16)
            for h in range(H):
                q_s[i, 2*D*h:2*D*h+D] = qh[D*h:D*h+D]
                q_s[i, 2*D*h+D:2*D*h+2*D] = ql[D*h:D*h+D]
                v_s[i, h, 0:D] = v[D*h:D*h+D]
                v_s[i, h, D:2*D] = ones
            g_s[i] = jax.nn.sigmoid(p[2*C:3*C] + bg_ref[...])
            return 0
        lax.fori_loop(0, R, prep, 0)

    q0 = pl.multiple_of(jb * QB, QB)
    zero = jnp.zeros((2*D, QB), BF16)
    for h in range(H):
        for c in range(0, N, KC):
            bias_s[c:c+KC] = bias_ref[h, c:c+KC].astype(F32) * LOG2E + mask_ref[c:c+KC, 0:1]
        def row(i, _):
            qw = q_s[i, 2*D*h:2*D*(h+1), pl.ds(q0, QB)]
            w = jnp.concatenate([zero]*h + [qw] + [zero]*(H-1-h), axis=0)
            m = None
            for c in range(0, N, KC):
                s = jnp.dot(k_s[i, c:c+KC], w, preferred_element_type=F32) + bias_s[c:c+KC]
                s_s[c:c+KC] = s
                mc = jnp.max(s.reshape(KC//8, 8, QB), axis=0)
                m = mc if m is None else jnp.maximum(m, mc)
            m = jnp.max(m, axis=0, keepdims=True)
            acc = None
            for c in range(0, N, KC):
                e = jnp.exp2(s_s[c:c+KC] - m).astype(BF16)
                a = jnp.dot(v_s[i, h, :, c:c+KC], e, preferred_element_type=F32)
                acc = a if acc is None else acc + a
            o = acc[0:D] / acc[D:D+1]
            o_s[i, D*h:D*h+D] = (g_s[i, D*h:D*h+D, pl.ds(q0, QB)] * o).astype(BF16)
            return 0
        lax.fori_loop(0, R, row, 0)

    def fin(i, _):
        u = jnp.dot(wo_ref[0:C, 0:C], o_s[i], preferred_element_type=F32) + bo_ref[...]
        zn = (z_ref[i, :, pl.ds(q0, QB)].astype(F32) + u).astype(BF16)
        out_ref[i] = zn
        y_s[pl.ds(pl.multiple_of(i*C, C), C)] = _ln_t(zn.astype(F32), lnn_ref[:, 0:1], lnn_ref[:, 1:2])
        return 0
    lax.fori_loop(0, R, fin, 0)
    bnext_ref[...] = jnp.dot(wbn_ref[...], y_s[...], preferred_element_type=F32).astype(BF16)

def attention_safe(z, bias, mask, lnw, wqvt, wk2, bg, wo, bo, lnn, wbn, QB=256, KC=256):
    R, C, N = z.shape
    H = bias.shape[0]
    full = lambda a: pl.BlockSpec(a.shape, lambda j: (0,)*a.ndim, pipeline_mode=pl.Buffered(1))
    return pl.pallas_call(
        functools.partial(safe_kernel, R, N, C, H, QB, KC),
        grid=(N//QB,),
        in_specs=[full(z), pl.BlockSpec((H, N, QB), lambda j: (0, 0, j)), full(mask), full(lnw), full(wqvt), full(wk2),
                  full(bg), full(wo), full(bo), full(lnn), full(wbn)],
        out_specs=[pl.BlockSpec((R, C, QB), lambda j: (0, 0, j)), pl.BlockSpec((H*R, QB), lambda j: (0, j))],
        out_shape=[jax.ShapeDtypeStruct((R, C, N), BF16), jax.ShapeDtypeStruct((H*R, N), BF16)],
        scratch_shapes=[pltpu.VMEM((R, N, 2*C), BF16), pltpu.VMEM((R, 2*C, N), BF16), pltpu.VMEM((R, H, 2*(C//H), N), BF16),
                        pltpu.VMEM((R, C, N), F32), pltpu.VMEM((R, C, QB), BF16), pltpu.VMEM((R*C, QB), BF16),
                        pltpu.VMEM((N, QB), F32), pltpu.VMEM((N, QB), F32)],
        compiler_params=pltpu.CompilerParams(dimension_semantics=("arbitrary",), vmem_limit_bytes=60*2**20),
        name="att_safe",
    )(z, bias, mask, lnw, wqvt, wk2, bg, wo, bo, lnn, wbn)


def _ln_rows(x, w):
    x = x.astype(F32)
    mu = jnp.mean(x, axis=-1, keepdims=True)
    var = jnp.mean(jnp.square(x - mu), axis=-1, keepdims=True)
    y = (x - mu) * lax.rsqrt(var + EPS)
    return (y * w[0].astype(F32) + w[1].astype(F32)).astype(BF16)


def _safe_to_skip_max(ws):
    ln_w, w_in, b_g, w_b, w_o, b_o = (a.astype(F32) for a in ws)
    L, P, C, H = w_b.shape
    D = C // H
    g, b = ln_w[:, :, 0], ln_w[:, :, 1]
    w = w_in.reshape(L, P, C, 4, H, D)[:, :, :, 0:3]
    wg = w * g[:, :, :, None, None, None]
    gram = jnp.sum(wg[..., :, None] * wg[..., None, :], axis=2)
    gram2 = jnp.sum(gram[..., :, :, None] * gram[..., None, :, :], axis=-2)
    lam = jnp.sqrt(jnp.max(jnp.sum(jnp.abs(gram2), axis=-1), axis=-1))
    off = jnp.sqrt(jnp.sum(jnp.square(jnp.sum(w * b[:, :, :, None, None, None], axis=2)), axis=-1))
    n = (jnp.sqrt(lam) * C ** 0.5 + off) * 1.02
    nb = jnp.sqrt(jnp.sum(jnp.square(w_b * g[..., None]), axis=2)) * C ** 0.5 + jnp.abs(jnp.sum(w_b * b[..., None], axis=2))
    s = LOG2E * (n[:, :, 0] * n[:, :, 1] * D ** -0.5 + nb * 1.02)
    ok = (s <= 100.0) & (n[:, :, 2] <= 2.0 ** 14)
    return jnp.all(ok, axis=-1)


def solution(mesh):
    def local(zl, res_mask, ln_w, w_in, b_g, w_b, w_o, b_o):
        R, N, C = zl.shape
        H = w_b.shape[-1]
        G = N // R
        mask = jnp.broadcast_to(jnp.where(res_mask > 0, 0.0, NEG).astype(F32)[:, None], (N, 128))
        ws = (ln_w, w_in, b_g, w_b, w_o, b_o)
        ok = _safe_to_skip_max(ws)
        passes = [(l, p) for l in range(ln_w.shape[0]) for p in range(2)]
        sets = [prep_weights(*(a[l, p] for a in ws), R) for l, p in passes]

        y = _ln_rows(zl, ln_w[0, 0])
        b = jnp.einsum('jkc,ch->hjk', y, w_b[0, 0], preferred_element_type=F32).astype(BF16)
        bias = jnp.swapaxes(lax.all_gather(b, 'dap', axis=1, tiled=True), 1, 2)
        z = jnp.swapaxes(zl, 1, 2)
        for n, (l, p) in enumerate(passes):
            lnw, wqvt, wk2, bg, wo, bo, _ = sets[n]
            nxt = sets[(n+1) % len(sets)]
            z, bn = lax.cond(ok[l, p], attention, attention_safe, z, bias, mask, lnw, wqvt, wk2, bg, wo, bo, nxt[0], nxt[6])
            x = jnp.transpose(z.reshape(R, C, G, R), (2, 3, 0, 1))
            x = lax.all_to_all(x, 'dap', 0, 0, tiled=True)
            if n+1 < len(passes):
                bias = lax.all_gather(bn.reshape(H, R, N), 'dap', axis=1, tiled=True)
                z = jnp.transpose(x, (1, 3, 0, 2)).reshape(R, C, N)
        return jnp.transpose(x, (1, 0, 2, 3)).reshape(R, N, C)

    rows = P(('data', 'dap'))
    return jax.shard_map(local, mesh=mesh,
                         in_specs=(rows, P('data'), P(), P(), P(), P(), P(), P()),
                         out_specs=rows, check_vma=False)
```

```python
import functools, math
import jax, jax.numpy as jnp
from jax import lax
from jax.experimental import pallas as pl
from jax.experimental.pallas import tpu as pltpu
from jax.sharding import PartitionSpec as P
F32=jnp.float32; BF16=jnp.bfloat16
EPS=1e-5; NEG=-1e9
LOG2E=1.4426950408889634
MX=256

def _ln_t(x, gamma, beta):
    mu = jnp.mean(x, axis=0, keepdims=True)
    d = x - mu
    var = jnp.mean(d*d, axis=0, keepdims=True)
    return (d * lax.rsqrt(var + EPS) * gamma + beta).astype(BF16)

def fast_kernel(R, N, C, H, LAG, NR, OA, FD,
               z_ref, bias_ref, mask_ref, lnw_ref, wqvt_ref, wk2_ref, bg_ref, wo_ref, bo_ref, lnn_ref, wbn_ref,
               out_ref, bnext_ref,
               k_s, q_s, v_s, g_s, o_s, y_s, bias_s, x_s, zt_s, send_sem, recv_sem, own_sem):
    jb = pl.program_id(0)
    me = lax.axis_index('dap')
    n_dev = lax.axis_size('dap')
    D = C // H
    QB = MX
    KC = 128

    @pl.when(jb == 0)
    def _():
        barrier = pltpu.get_barrier_semaphore()
        def greet(k, _):
            pl.semaphore_signal(barrier, inc=1, device_id={'dap': lax.rem(me + k, n_dev)}, device_id_type=pl.DeviceIdType.MESH)
            return 0
        lax.fori_loop(1, n_dev, greet, 0)
        pl.semaphore_wait(barrier, n_dev - 1)
    CH = N // KC
    q0 = pl.multiple_of(jb * QB, QB)

    def body(*accs):
        sacc = [accs[0:NR], accs[NR:2*NR]]
        oacc = [accs[2*NR:2*NR+OA], accs[2*NR+OA:2*NR+2*OA]]
        z128 = jnp.zeros((KC, MX-KC), BF16)
        zrow = lambda n: jnp.zeros((n, MX), BF16)

        @pl.when(jb == 0)
        def _():
            def prep(i, _):
                y = _ln_t(z_ref[i].astype(F32), lnw_ref[:, 0:1], lnw_ref[:, 1:2])
                yt = jnp.concatenate([y, jnp.zeros((KC-C, N), BF16)], axis=0).T
                for j in range(N//MX):
                    m = j % 2
                    cs = slice(j*MX, (j+1)*MX)
                    pltpu.matmul_push_rhs(jnp.concatenate([y[:, cs], zrow(MX-C)], axis=0), staging_register=0, mxu_index=m)
                    pltpu.matmul_acc_lhs(sacc[m][0], wqvt_ref[0:KC], load_staged_rhs=0)
                    pltpu.matmul_acc_lhs(sacc[m][1], wqvt_ref[KC:2*KC])
                    pltpu.matmul_push_rhs(wk2_ref[...], staging_register=1, mxu_index=m)
                    for r in range(2):
                        kk = jnp.concatenate([yt[j*MX+r*KC:j*MX+(r+1)*KC], z128], axis=1)
                        pltpu.matmul_acc_lhs(sacc[m][2+r], kk, load_staged_rhs=1 if r == 0 else None)
                    qv = pltpu.matmul_pop(sacc[m][0])
                    q = qv[0:C].astype(BF16).astype(F32) * (LOG2E * D ** -0.5)
                    qh = q.astype(BF16)
                    ql = (q - qh.astype(F32)).astype(BF16)
                    for h in range(H):
                        q_s[i, 2*D*h:2*D*h+D, cs] = qh[D*h:D*h+D]
                        q_s[i, 2*D*h+D:2*D*h+2*D, cs] = ql[D*h:D*h+D]
                    v_s[i, :, cs] = qv[C:2*C].astype(BF16)
                    t = pltpu.matmul_pop(sacc[m][1])
                    g_s[i, :, cs] = jax.nn.sigmoid(t[0:C] + bg_ref[...])
                    for r in range(2):
                        k_s[i, j*MX+r*KC:j*MX+(r+1)*KC] = pltpu.matmul_pop(sacc[m][2+r])[:, 0:2*C].astype(BF16)
                return 0
            lax.fori_loop(0, R, prep, 0)

        for h in range(H):
            for c in range(CH):
                sl = slice(c*KC, (c+1)*KC)
                for w in range(2):
                    bias_s[h, sl, w*128:(w+1)*128] = bias_ref[h, sl, w*128:(w+1)*128].astype(F32) * LOG2E + mask_ref[sl]

        zp = jnp.zeros((KC, QB), BF16)
        zv = jnp.zeros((2*D, MX-KC), BF16)
        zq = jnp.zeros((2*D, QB), BF16)
        ones = jnp.where(lax.broadcasted_iota(jnp.int32, (D, KC), 0) == 0, 1.0, 0.0).astype(BF16)
        steps = [(h, c) for h in range(H) for c in range(CH)]
        S = len(steps)

        def pair(t, _):
            es = {}
            def tile(n):
                for m in range(2):
                    p = es.pop((n, m)) if n >= 0 else zp
                    if n+LAG < S:
                        h, c = steps[n+LAG]
                        w = jnp.concatenate([zq]*h + [q_s[2*t+m, 2*D*h:2*D*(h+1), pl.ds(q0, QB)]] + [zq]*(H-1-h), axis=0)
                    else:
                        w = zp
                    pltpu.matmul_push_rhs(jnp.concatenate([p, w], axis=0), staging_register=n % 2, mxu_index=m)
            def accum(n):
                for m in range(2):
                    ld = n % 2
                    if n+LAG < S:
                        h, c = steps[n+LAG]
                        kk = jnp.concatenate([z128, k_s[2*t+m, c*KC:(c+1)*KC]], axis=1)
                        pltpu.matmul_acc_lhs(sacc[m][(n+LAG) % NR], kk, load_staged_rhs=ld)
                        ld = None
                    if n >= 0:
                        h, c = steps[n]
                        vv = jnp.concatenate([v_s[2*t+m, D*h:D*h+D, c*KC:(c+1)*KC], ones], axis=0)
                        pltpu.matmul_acc_lhs(oacc[m][h % OA], jnp.concatenate([vv, zv], axis=1), load_staged_rhs=ld)
            def ex(n):
                h, c = steps[n]
                b = bias_s[h, c*KC:(c+1)*KC]
                for m in range(2):
                    es[n, m] = jnp.exp2(pltpu.matmul_pop(sacc[m][n % NR]) + b).astype(BF16)
            def fin(n):
                h, c = steps[n]
                if c == CH-1:
                    for m in range(2):
                        i = 2*t+m
                        a = pltpu.matmul_pop(oacc[m][h % OA])
                        o_s[i, D*h:D*h+D] = (g_s[i, D*h:D*h+D, pl.ds(q0, QB)] * (a[0:D] / a[D:D+1])).astype(BF16)
            for n in range(-LAG, S):
                if n >= 0: ex(n)
                tile(n); accum(n)
                if n-FD >= 0: fin(n-FD)
            for n in range(S-FD, S): fin(n)
            return 0
        lax.fori_loop(0, R//2, pair, 0)

        def upd(t, _):
            for m in range(2):
                pltpu.matmul_push_rhs(jnp.concatenate([o_s[2*t+m], zrow(MX-C)], axis=0), staging_register=0, mxu_index=m)
                pltpu.matmul_acc_lhs(sacc[m][0], wo_ref[...], load_staged_rhs=0)
            for m in range(2):
                i = 2*t+m
                u = pltpu.matmul_pop(sacc[m][0])[0:C] + bo_ref[...]
                zn = (z_ref[i, :, pl.ds(q0, QB)].astype(F32) + u).astype(BF16)
                zt_s[pl.ds(pl.multiple_of(i*C, C), C)] = zn
                y_s[pl.ds(pl.multiple_of(i*C, C), C)] = _ln_t(zn.astype(F32), lnn_ref[:, 0:1], lnn_ref[:, 1:2])
            return 0
        lax.fori_loop(0, R//2, upd, 0)
        x_s[pl.ds(jb * (QB//R), QB//R)] = zt_s[...].T.reshape(QB//R, R, R*C)
        for m in range(2):
            pltpu.matmul_push_rhs(y_s[m*MX:(m+1)*MX], staging_register=0, mxu_index=m)
            pltpu.matmul_acc_lhs(oacc[m][0], wbn_ref[:, m*MX:(m+1)*MX], load_staged_rhs=0)
        bnext_ref[...] = (pltpu.matmul_pop(oacc[0][0]) + pltpu.matmul_pop(oacc[1][0])).astype(BF16)

        def send(k, _):
            d = jb * (QB//R) + k
            @pl.when(d != me)
            def _():
                pltpu.make_async_remote_copy(x_s.at[d], out_ref.at[me], send_sem, recv_sem,
                                             device_id={'dap': d}, device_id_type=pl.DeviceIdType.MESH).start()
            @pl.when(d == me)
            def _():
                pltpu.make_async_copy(x_s.at[d], out_ref.at[d], own_sem).start()
            return 0
        lax.fori_loop(0, QB//R, send, 0)

        @pl.when(jb == pl.num_programs(0) - 1)
        def _():
            pltpu.make_async_copy(x_s.at[0], out_ref.at[0], own_sem).wait()
            pltpu.make_async_copy(x_s.at[pl.ds(0, n_dev-1)], out_ref.at[pl.ds(0, n_dev-1)], send_sem).wait()
            pltpu.make_async_copy(x_s.at[pl.ds(0, n_dev-1)], out_ref.at[pl.ds(0, n_dev-1)], recv_sem).wait()

    pl.run_scoped(body, *[pltpu.ACC(m)((KC, MX), F32) for m in range(2) for _ in range(NR)],
                  *[pltpu.ACC(m)((2*D, MX), F32) for m in range(2) for _ in range(OA)])

def attention(z, bias, mask, lnw, wqvt, wk2, bg, wo, bo, lnn, wbn, LAG=4, NR=5, OA=2, FD=3, FL={}):
    R, C, N = z.shape
    H = bias.shape[0]
    QB = MX
    full = lambda a: pl.BlockSpec(a.shape, lambda j: (0,)*a.ndim, pipeline_mode=pl.Buffered(1))
    return pl.pallas_call(
        functools.partial(fast_kernel, R, N, C, H, LAG, NR, OA, FD),
        grid=(N//QB,),
        in_specs=[full(z), pl.BlockSpec((H, N, QB), lambda j: (0, 0, j)), full(mask), full(lnw), full(wqvt), full(wk2),
                  full(bg), full(wo), full(bo), full(lnn), full(wbn)],
        out_specs=[pl.BlockSpec(memory_space=pl.ANY), pl.BlockSpec((H*R, QB), lambda j: (0, j))],
        out_shape=[jax.ShapeDtypeStruct((N//R, R, R*C), BF16), jax.ShapeDtypeStruct((H*R, N), BF16)],
        scratch_shapes=[pltpu.VMEM((R, N, 2*C), BF16), pltpu.VMEM((R, 2*C, N), BF16), pltpu.VMEM((R, C, N), BF16),
                        pltpu.VMEM((R, C, N), F32), pltpu.VMEM((R, C, QB), BF16), pltpu.VMEM((R*C, QB), BF16),
                        pltpu.VMEM((H, N, QB), F32), pltpu.VMEM((N//R, R, R*C), BF16), pltpu.VMEM((R*C, QB), BF16),
                        pltpu.SemaphoreType.DMA, pltpu.SemaphoreType.DMA, pltpu.SemaphoreType.DMA],
        compiler_params=pltpu.CompilerParams(dimension_semantics=("arbitrary",), vmem_limit_bytes=48*2**20, flags=FL, collective_id=0, has_side_effects=True),
        name="att_fast",
    )(z, bias, mask, lnw, wqvt, wk2, bg, wo, bo, lnn, wbn)

def prep_weights(ln_w, w_in, b_g, w_b, w_o, b_o, R):
    C = w_o.shape[0]; H = w_b.shape[1]; D = C // H
    lnw = ln_w.astype(F32).T
    wq, wk, wv, wt = (w_in[:, i*C:(i+1)*C] for i in range(4))
    wqvt = jnp.pad(jnp.concatenate([wq, wv, wt], axis=1).T, ((0, MX-3*C), (0, MX-C)))
    wk2 = jnp.concatenate([wk.reshape(C, H, 1, D)]*2, axis=2).reshape(C, 2*C)
    wk2 = jnp.pad(wk2, ((0, MX-C), (0, MX-2*C)))
    bg = b_g.astype(F32).reshape(C, 1)
    bo = b_o.astype(F32).reshape(C, 1)
    eye = jnp.eye(R, dtype=w_b.dtype)
    wbn = (w_b.T[:, None, None, :] * eye[None, :, :, None]).reshape(H*R, R*C)
    wo = jnp.pad(w_o.T, ((0, 2*C-C), (0, MX-C)))
    return lnw, wqvt, wk2, bg, wo, bo, wbn


def safe_kernel(R, N, C, H, QB, KC,
               z_ref, bias_ref, mask_ref, lnw_ref, wqvt_ref, wk2_ref, bg_ref, wo_ref, bo_ref, lnn_ref, wbn_ref,
               out_ref, bnext_ref,
               k_s, q_s, v_s, g_s, o_s, y_s, bias_s, s_s, x_s, zt_s, send_sem, recv_sem, own_sem):
    jb = pl.program_id(0)
    me = lax.axis_index('dap')
    n_dev = lax.axis_size('dap')

    @pl.when(jb == 0)
    def _():
        barrier = pltpu.get_barrier_semaphore()
        def greet(k, _):
            pl.semaphore_signal(barrier, inc=1, device_id={'dap': lax.rem(me + k, n_dev)}, device_id_type=pl.DeviceIdType.MESH)
            return 0
        lax.fori_loop(1, n_dev, greet, 0)
        pl.semaphore_wait(barrier, n_dev - 1)
    D = C // H

    @pl.when(jb == 0)
    def _():
        rows = lax.broadcasted_iota(jnp.int32, (16, N), 0)
        ones = jnp.where(rows == 0, 1.0, 0.0).astype(BF16)
        def prep(i, _):
            x = z_ref[i].astype(F32)
            y = _ln_t(x, lnw_ref[:, 0:1], lnw_ref[:, 1:2])
            p = jnp.dot(wqvt_ref[0:3*C, 0:C], y, preferred_element_type=F32)
            yt = y.T
            k2 = jnp.dot(yt, wk2_ref[0:C, 0:2*C], preferred_element_type=F32).astype(BF16)
            k_s[i] = k2
            q = p[0:C].astype(BF16).astype(F32) * (LOG2E * D ** -0.5)
            qh = q.astype(BF16)
            ql = (q - qh.astype(F32)).astype(BF16)
            v = p[C:2*C].astype(BF16)
            for h in range(H):
                q_s[i, 2*D*h:2*D*h+D] = qh[D*h:D*h+D]
                q_s[i, 2*D*h+D:2*D*h+2*D] = ql[D*h:D*h+D]
                v_s[i, h, 0:D] = v[D*h:D*h+D]
                v_s[i, h, D:2*D] = ones
            g_s[i] = jax.nn.sigmoid(p[2*C:3*C] + bg_ref[...])
            return 0
        lax.fori_loop(0, R, prep, 0)

    q0 = pl.multiple_of(jb * QB, QB)
    zero = jnp.zeros((2*D, QB), BF16)
    for h in range(H):
        for c in range(0, N, KC):
            bias_s[c:c+KC] = bias_ref[h, c:c+KC].astype(F32) * LOG2E + mask_ref[c:c+KC, 0:1]
        def row(i, _):
            qw = q_s[i, 2*D*h:2*D*(h+1), pl.ds(q0, QB)]
            w = jnp.concatenate([zero]*h + [qw] + [zero]*(H-1-h), axis=0)
            m = None
            for c in range(0, N, KC):
                s = jnp.dot(k_s[i, c:c+KC], w, preferred_element_type=F32) + bias_s[c:c+KC]
                s_s[c:c+KC] = s
                mc = jnp.max(s.reshape(KC//8, 8, QB), axis=0)
                m = mc if m is None else jnp.maximum(m, mc)
            m = jnp.max(m, axis=0, keepdims=True)
            acc = None
            for c in range(0, N, KC):
                e = jnp.exp2(s_s[c:c+KC] - m).astype(BF16)
                a = jnp.dot(v_s[i, h, :, c:c+KC], e, preferred_element_type=F32)
                acc = a if acc is None else acc + a
            o = acc[0:D] / acc[D:D+1]
            o_s[i, D*h:D*h+D] = (g_s[i, D*h:D*h+D, pl.ds(q0, QB)] * o).astype(BF16)
            return 0
        lax.fori_loop(0, R, row, 0)

    def fin(i, _):
        u = jnp.dot(wo_ref[0:C, 0:C], o_s[i], preferred_element_type=F32) + bo_ref[...]
        zn = (z_ref[i, :, pl.ds(q0, QB)].astype(F32) + u).astype(BF16)
        zt_s[pl.ds(pl.multiple_of(i*C, C), C)] = zn
        y_s[pl.ds(pl.multiple_of(i*C, C), C)] = _ln_t(zn.astype(F32), lnn_ref[:, 0:1], lnn_ref[:, 1:2])
        return 0
    lax.fori_loop(0, R, fin, 0)
    bnext_ref[...] = jnp.dot(wbn_ref[...], y_s[...], preferred_element_type=F32).astype(BF16)
    x_s[pl.ds(jb * (QB//R), QB//R)] = zt_s[...].T.reshape(QB//R, R, R*C)

    def send(k, _):
        d = jb * (QB//R) + k
        @pl.when(d != me)
        def _():
            pltpu.make_async_remote_copy(x_s.at[d], out_ref.at[me], send_sem, recv_sem,
                                         device_id={'dap': d}, device_id_type=pl.DeviceIdType.MESH).start()
        @pl.when(d == me)
        def _():
            pltpu.make_async_copy(x_s.at[d], out_ref.at[d], own_sem).start()
        return 0
    lax.fori_loop(0, QB//R, send, 0)

    @pl.when(jb == pl.num_programs(0) - 1)
    def _():
        pltpu.make_async_copy(x_s.at[0], out_ref.at[0], own_sem).wait()
        pltpu.make_async_copy(x_s.at[pl.ds(0, n_dev-1)], out_ref.at[pl.ds(0, n_dev-1)], send_sem).wait()
        pltpu.make_async_copy(x_s.at[pl.ds(0, n_dev-1)], out_ref.at[pl.ds(0, n_dev-1)], recv_sem).wait()


def attention_safe(z, bias, mask, lnw, wqvt, wk2, bg, wo, bo, lnn, wbn, QB=256, KC=256):
    R, C, N = z.shape
    H = bias.shape[0]
    full = lambda a: pl.BlockSpec(a.shape, lambda j: (0,)*a.ndim, pipeline_mode=pl.Buffered(1))
    return pl.pallas_call(
        functools.partial(safe_kernel, R, N, C, H, QB, KC),
        grid=(N//QB,),
        in_specs=[full(z), pl.BlockSpec((H, N, QB), lambda j: (0, 0, j)), full(mask), full(lnw), full(wqvt), full(wk2),
                  full(bg), full(wo), full(bo), full(lnn), full(wbn)],
        out_specs=[pl.BlockSpec(memory_space=pl.ANY), pl.BlockSpec((H*R, QB), lambda j: (0, j))],
        out_shape=[jax.ShapeDtypeStruct((N//R, R, R*C), BF16), jax.ShapeDtypeStruct((H*R, N), BF16)],
        scratch_shapes=[pltpu.VMEM((R, N, 2*C), BF16), pltpu.VMEM((R, 2*C, N), BF16), pltpu.VMEM((R, H, 2*(C//H), N), BF16),
                        pltpu.VMEM((R, C, N), F32), pltpu.VMEM((R, C, QB), BF16), pltpu.VMEM((R*C, QB), BF16),
                        pltpu.VMEM((N, QB), F32), pltpu.VMEM((N, QB), F32), pltpu.VMEM((N//R, R, R*C), BF16), pltpu.VMEM((R*C, QB), BF16),
                        pltpu.SemaphoreType.DMA, pltpu.SemaphoreType.DMA, pltpu.SemaphoreType.DMA],
        compiler_params=pltpu.CompilerParams(dimension_semantics=("arbitrary",), vmem_limit_bytes=60*2**20, collective_id=0, has_side_effects=True),
        name="att_safe",
    )(z, bias, mask, lnw, wqvt, wk2, bg, wo, bo, lnn, wbn)


def _ln_rows(x, w):
    x = x.astype(F32)
    mu = jnp.mean(x, axis=-1, keepdims=True)
    var = jnp.mean(jnp.square(x - mu), axis=-1, keepdims=True)
    y = (x - mu) * lax.rsqrt(var + EPS)
    return (y * w[0].astype(F32) + w[1].astype(F32)).astype(BF16)


def _safe_to_skip_max(ws):
    ln_w, w_in, b_g, w_b, w_o, b_o = (a.astype(F32) for a in ws)
    L, P, C, H = w_b.shape
    D = C // H
    g, b = ln_w[:, :, 0], ln_w[:, :, 1]
    w = w_in.reshape(L, P, C, 4, H, D)[:, :, :, 0:3]
    wg = w * g[:, :, :, None, None, None]
    gram = jnp.sum(wg[..., :, None] * wg[..., None, :], axis=2)
    gram2 = jnp.sum(gram[..., :, :, None] * gram[..., None, :, :], axis=-2)
    lam = jnp.sqrt(jnp.max(jnp.sum(jnp.abs(gram2), axis=-1), axis=-1))
    off = jnp.sqrt(jnp.sum(jnp.square(jnp.sum(w * b[:, :, :, None, None, None], axis=2)), axis=-1))
    n = (jnp.sqrt(lam) * C ** 0.5 + off) * 1.02
    nb = jnp.sqrt(jnp.sum(jnp.square(w_b * g[..., None]), axis=2)) * C ** 0.5 + jnp.abs(jnp.sum(w_b * b[..., None], axis=2))
    s = LOG2E * (n[:, :, 0] * n[:, :, 1] * D ** -0.5 + nb * 1.02)
    ok = (s <= 100.0) & (n[:, :, 2] <= 2.0 ** 14)
    return jnp.all(ok, axis=-1)


def solution(mesh):
    def local(zl, res_mask, ln_w, w_in, b_g, w_b, w_o, b_o):
        R, N, C = zl.shape
        H = w_b.shape[-1]
        G = N // R
        mask = jnp.broadcast_to(jnp.where(res_mask > 0, 0.0, NEG).astype(F32)[:, None], (N, 128))
        ws = (ln_w, w_in, b_g, w_b, w_o, b_o)
        ok = _safe_to_skip_max(ws)
        passes = [(l, p) for l in range(ln_w.shape[0]) for p in range(2)]
        sets = [prep_weights(*(a[l, p] for a in ws), R) for l, p in passes]

        def safe(*args):
            z, bn = attention_safe(*args)
            x = jnp.transpose(z.reshape(R, C, G, R), (2, 3, 0, 1)).reshape(G, R, R*C)
            return lax.all_to_all(x, 'dap', 0, 0, tiled=True), bn

        y = _ln_rows(zl, ln_w[0, 0])
        b = jnp.einsum('jkc,ch->hjk', y, w_b[0, 0], preferred_element_type=F32).astype(BF16)
        bias = jnp.swapaxes(lax.all_gather(b, 'dap', axis=1, tiled=True), 1, 2)
        z = jnp.swapaxes(zl, 1, 2)
        for n, (l, p) in enumerate(passes):
            lnw, wqvt, wk2, bg, wo, bo, _ = sets[n]
            nxt = sets[(n+1) % len(sets)]
            x, bn = attention_safe(z, bias, mask, lnw, wqvt, wk2, bg, wo, bo, nxt[0], nxt[6])
            x = x.reshape(G, R, R, C)
            if n+1 < len(passes):
                bias = lax.all_gather(bn.reshape(H, R, N), 'dap', axis=1, tiled=True)
                z = jnp.transpose(x, (1, 3, 0, 2)).reshape(R, C, N)
        return jnp.transpose(x, (1, 0, 2, 3)).reshape(R, N, C)

    rows = P(('data', 'dap'))
    return jax.shard_map(local, mesh=mesh,
                         in_specs=(rows, P('data'), P(), P(), P(), P(), P(), P()),
                         out_specs=rows, check_vma=False)
```

```python
import functools
import jax
import jax.numpy as jnp
from jax import lax
from jax.experimental import pallas as pl
from jax.experimental.pallas import tpu as pltpu
from jax.sharding import PartitionSpec as P

F32 = jnp.float32
BF16 = jnp.bfloat16
EPS = 1e-5
NEG = -1e9
LOG2E = 1.4426950408889634
TZ, TY, TX, TC = 4, 4, 4, 2
PARTS = (((2, 1, 0), 0, 3), ((1, 0, 2), 3, 3), ((0, 2, 1), 6, 2))
MESH = pl.DeviceIdType.MESH


def _ln_t(x, gamma, beta):
    mu = jnp.mean(x, axis=0, keepdims=True)
    d = x - mu
    var = jnp.mean(d*d, axis=0, keepdims=True)
    return (d * lax.rsqrt(var + EPS) * gamma + beta).astype(BF16)


def mega_kernel(R, N, C, H, LAG, ME,
                z_ref, mask_ref, lnw_ref, wqvt_ref, wk2_ref, bg_ref, wo_ref, bo_ref, wbn_ref,
                out_ref,
                k_s, q_s, v_s, g_s, z_s, o_s, y_s, zt_s, bias_s, x_s, r_s, G,
                a2a_send, a2a_recv, own_sem, ag_send, ag_recv):
    ps, jb = pl.program_id(0), pl.program_id(1)
    n_pass, n_blk = lnw_ref.shape[0], 4
    others = pl.ds(0, TZ*TY*TX*TC-1)
    me = lax.axis_index('dap')
    n_dev = TZ*TY*TX*TC
    D = C // H
    QB = N // 4
    KC = 128
    CH = N // KC
    DB = QB // R
    par, nxt = lax.rem(ps, 2), lax.rem(ps + 1, 2)
    q0 = pl.multiple_of(jb * QB, QB)
    core = lax.rem(me, TC)
    at = (lax.div(me, TY*TX*TC), lax.rem(lax.div(me, TX*TC), TY), lax.rem(lax.div(me, TC), TX))

    def dev(z, y, x, c):
        return {'dap': ((z*TY + y)*TX + x)*TC + c}

    def moved(axis, by):
        p = list(at)
        p[axis] = lax.rem(p[axis] + by, 4)
        return p

    def chunk(g, b, sel, u0, nu):
        return G.at[g, b, sel[0], sel[1], sel[2], core, pl.ds(u0, nu)]

    def copy(g, b, k, sel, u0, nu, to, c):
        r = chunk(g, b, sel, u0, nu)
        return pltpu.make_async_remote_copy(r, r, ag_send.at[g, b, k], ag_recv.at[g, b, k],
                                            device_id=dev(*to, c), device_id_type=MESH)

    def landed(g, b, k, sem):
        sel = ((0, 0, pl.ds(0, 3)), (0, pl.ds(0, 3), slice(None)), (pl.ds(0, 2), slice(None), slice(None)),
               (0, slice(None), slice(None)), (slice(None),)*3)[k]
        r = G.at[g, b, sel[0], sel[1], sel[2], 0]
        pltpu.make_async_copy(r, r, sem.at[g, b, k]).wait()

    def stage(k, g, b):
        if k > 0:
            landed(g, b, k-1, ag_recv)
        if k == 5:
            for j in range(5):
                landed(g, b, j, ag_send)
            return
        if k == 4:
            r = G.at[g, b, :, :, :, core]
            pltpu.make_async_remote_copy(r, r, ag_send.at[g, b, 4], ag_recv.at[g, b, 4],
                                         device_id=dev(*at, 1-core), device_id_type=MESH).start()
            return
        for (a0, a1, a2), u0, nu in PARTS:
            sel = list(at)
            if k == 0:
                for by in (1, 3, 2):
                    copy(g, b, k, sel, u0, nu, moved(a0, by), core).start()
            elif k == 1:
                sel[a0] = slice(None)
                for by in (1, 3, 2):
                    copy(g, b, k, sel, u0, nu, moved(a1, by), core).start()
            elif k == 2:
                sel[a0] = sel[a1] = slice(None)
                for by in (1, 3):
                    copy(g, b, k, sel, u0, nu, moved(a2, by), core).start()
            else:
                for by, half in ((1, 0), (3, 2)):
                    sel[a0] = slice(None)
                    sel[a1] = pl.ds(half, 2)
                    sel[a2] = lax.rem(at[a2] + 4 - by, 4)
                    copy(g, b, k, sel, u0, nu, moved(a2, by), core).start()

    def slot(s, p, lo, hi):
        for k in range(6):
            b = s - k
            if hi - k >= 0 and lo - k < n_blk:
                @pl.when((b >= 0) & (b < n_blk) & (p < n_pass-1))
                def _():
                    stage(k, lax.rem(p + 1, 2), b)
            if lo - k + 6 < 4:
                @pl.when((b < 0) & (b + 6 < n_blk) & (p >= 1))
                def _():
                    stage(k, lax.rem(p, 2), b + 6)

    def put_bias(g, b, rows):
        for h in range(H):
            for t in range(2):
                G[g, b, at[0], at[1], at[2], core, 2*h+t] = rows[h*R:(h+1)*R, t*128:(t+1)*128]

    def bias_rows(p, y):
        return jnp.dot(wbn_ref[p], y, preferred_element_type=F32).astype(BF16)

    def prep(i, _):
        y = _ln_t(z_s[i].astype(F32), lnw_ref[ps, :, 0:1], lnw_ref[ps, :, 1:2])
        p = jnp.dot(wqvt_ref[ps], y, preferred_element_type=F32)
        k_s[i] = jnp.dot(y.T, wk2_ref[ps], preferred_element_type=F32).astype(BF16)
        q = p[0:C].astype(BF16).astype(F32) * (LOG2E * D ** -0.5)
        qh = q.astype(BF16)
        ql = (q - qh.astype(F32)).astype(BF16)
        for h in range(H):
            q_s[i, 2*D*h:2*D*h+D] = qh[D*h:D*h+D]
            q_s[i, 2*D*h+D:2*D*h+2*D] = ql[D*h:D*h+D]
        v_s[i] = p[C:2*C].astype(BF16)
        g_s[i] = jax.nn.sigmoid(p[2*C:3*C] + bg_ref[ps])
        return 0

    def unpack(w, _):
        t = r_s[par, pl.ds(w*16, 16)].reshape(128, R*C).astype(F32).T
        x = [t[i*C:(i+1)*C] for i in range(R)]
        lane = lax.broadcasted_iota(jnp.int32, (C, 128), 1)
        for bit in (1, 2, 4):
            odd = (lane & bit) != 0
            for i in range(R):
                if not i & bit:
                    a, b = x[i], x[i | bit]
                    x[i] = jnp.where(odd, pltpu.roll(b, bit, 1), a)
                    x[i | bit] = jnp.where(odd, b, pltpu.roll(a, 128-bit, 1))
        for i in range(R):
            z_s[i, :, pl.ds(pl.multiple_of(w*128, 128), 128)] = x[i].astype(BF16)
        return 0

    @pl.when((jb == 0) & (ps == 0))
    def _():
        barrier = pltpu.get_barrier_semaphore()
        def greet(k, _):
            pl.semaphore_signal(barrier, inc=1, device_id={'dap': lax.rem(me + k, n_dev)}, device_id_type=MESH)
            return 0
        lax.fori_loop(1, n_dev, greet, 0)
        def first(b, _):
            qs = pl.ds(pl.multiple_of(b*QB, QB), QB)
            for i in range(R):
                zb = z_ref[i, :, qs]
                z_s[i, :, qs] = zb
                y_s[i*C:(i+1)*C] = _ln_t(zb.astype(F32), lnw_ref[0, :, 0:1], lnw_ref[0, :, 1:2])
            put_bias(0, b, bias_rows(0, y_s[...]))
            return 0
        lax.fori_loop(0, n_blk, first, 0)
        pl.semaphore_wait(barrier, n_dev - 1)
        def gather(k):
            def each(b, _):
                stage(k, 0, b)
                return 0
            lax.fori_loop(0, n_blk, each, 0)
        gather(0)
        lax.fori_loop(0, R//2, prep, 0)
        gather(1)
        lax.fori_loop(R//2, R, prep, 0)
        for k in range(2, 6):
            gather(k)

    @pl.when((jb == 0) & (ps > 0))
    def _():
        pltpu.make_async_copy(r_s.at[par, others], r_s.at[par, others], a2a_recv.at[par]).wait()
        pltpu.make_async_copy(r_s.at[par, others], r_s.at[par, others], a2a_send).wait()
        lax.fori_loop(0, N//128, unpack, 0)
        lax.fori_loop(0, R//2, prep, 0)
        slot(4, ps-1, 4, 4)
        lax.fori_loop(R//2, R, prep, 0)
        slot(5, ps-1, 5, 5)

    @pl.when(ps == 0)
    def _():
        def each(h, _):
            for b in range(n_blk):
                for t in range(2):
                    v = G[0, b, jb, :, :, :, 2*h+t].reshape(QB, 128).astype(F32).T
                    rows = slice((2*b+t)*128, (2*b+t+1)*128)
                    for w in range(2):
                        bias_s[h, rows, w*128:(w+1)*128] = v[:, w*128:(w+1)*128] * LOG2E + mask_ref[rows]
            return 0
        lax.fori_loop(0, H, each, 0)

    @pl.when(ps > 0)
    def _():
        def each(h, _):
            for m in range(CH):
                for w in range(2):
                    v = G[par, jb, m//2, 2*(m % 2):2*(m % 2)+2, :, :, 2*h+w].reshape(128, 128).astype(F32)
                    bias_s[h, m*128:(m+1)*128, w*128:(w+1)*128] = v * LOG2E + mask_ref[m*128:(m+1)*128]
            return 0
        lax.fori_loop(0, H, each, 0)

    zl = jnp.zeros((KC, 256-2*C), BF16)
    zp = jnp.zeros((KC, QB), BF16)
    zv = jnp.zeros((2*D, 256-KC), BF16)
    zq = jnp.zeros((2*D, QB), BF16)
    ones = jnp.where(lax.broadcasted_iota(jnp.int32, (D, KC), 0) == 0, 1.0, 0.0).astype(BF16)
    steps = [(h, t, c) for h in range(H) for t in range(R//ME) for c in range(CH)]
    S = len(steps)
    es, ss, acc = {}, {}, [None]*ME
    for n in range(-LAG, S):
        if n >= 0:
            h, t, c = steps[n]
            b = bias_s[h, c*KC:(c+1)*KC]
            for m in range(ME):
                es[m] = jnp.exp2(ss.pop((n, m)) + b).astype(BF16)
        for m in range(ME):
            rows = []
            w = zp
            if n+LAG < S:
                h2, t2, c2 = steps[n+LAG]
                i2 = ME*t2+m
                w = jnp.concatenate([zq]*h2 + [q_s[i2, 2*D*h2:2*D*(h2+1), pl.ds(q0, QB)]] + [zq]*(H-1-h2), axis=0)
                rows.append(jnp.concatenate([zl, k_s[i2, c2*KC:(c2+1)*KC]], axis=1))
            if n >= 0:
                vv = jnp.concatenate([v_s[ME*t+m, D*h:D*h+D, c*KC:(c+1)*KC], ones], axis=0)
                rows.append(jnp.concatenate([vv, zv], axis=1))
            o = jnp.dot(jnp.concatenate(rows, axis=0), jnp.concatenate([es.pop(m) if n >= 0 else zp, w], axis=0),
                        preferred_element_type=F32)
            if n+LAG < S:
                ss[n+LAG, m] = o[0:KC]
            if n >= 0:
                i = ME*t+m
                o = o[-2*D:]
                acc[m] = o if c == 0 else acc[m] + o
                if c == CH-1:
                    a = acc[m][0:D] / acc[m][D:D+1]
                    o_s[i, D*h:D*h+D] = (g_s[i, D*h:D*h+D, pl.ds(q0, QB)] * a).astype(BF16)

    pn = lax.rem(ps + 1, n_pass)

    def upd(i, _):
        u = jnp.dot(wo_ref[ps], o_s[i], preferred_element_type=F32) + bo_ref[ps]
        zn = (z_s[i, :, pl.ds(q0, QB)].astype(F32) + u).astype(BF16)
        rows = pl.ds(pl.multiple_of(i*C, C), C)
        zt_s[rows] = zn
        y_s[rows] = _ln_t(zn.astype(F32), lnw_ref[pn, :, 0:1], lnw_ref[pn, :, 1:2])
        return 0
    lax.fori_loop(0, R, upd, 0)
    x_s[pl.ds(jb*DB, DB)] = zt_s[...].T.reshape(DB, R, R*C)

    @pl.when(ps < n_pass-1)
    def _():
        put_bias(nxt, jb, bias_rows(pn, y_s[...]))

    def send(k, _):
        d = jb*DB + k
        @pl.when(d != me)
        def _():
            pltpu.make_async_remote_copy(x_s.at[d], r_s.at[nxt, me], a2a_send, a2a_recv.at[nxt],
                                         device_id={'dap': d}, device_id_type=MESH).start()
        return 0
    lax.fori_loop(0, DB, send, 0)

    @pl.when((me >= jb*DB) & (me < (jb+1)*DB))
    def _():
        r_s[nxt, me] = x_s[me]
    slot(jb, ps, 0, 3)

    @pl.when((ps == n_pass-1) & (jb == n_blk-1))
    def _():
        pltpu.make_async_copy(r_s.at[nxt, others], r_s.at[nxt, others], a2a_recv.at[nxt]).wait()
        pltpu.make_async_copy(r_s.at[nxt, others], r_s.at[nxt, others], a2a_send).wait()
        out = pltpu.make_async_copy(r_s.at[nxt], out_ref, own_sem)
        out.start()
        out.wait()


def mega(z, mask, lnw, wqvt, wk2, bg, wo, bo, wbn, LAG=2, ME=4):
    R, C, N = z.shape
    n_pass = lnw.shape[0]
    H = wbn.shape[1] // R
    QB = N // 4
    full = lambda a: pl.BlockSpec(a.shape, lambda p, j: (0,)*a.ndim, pipeline_mode=pl.Buffered(1))
    args = (z, mask, lnw, wqvt, wk2, bg, wo, bo, wbn)
    flops = n_pass * (4*R*H*N*N*(C//H) + 2*R*N*C*6*C)
    return pl.pallas_call(
        functools.partial(mega_kernel, R, N, C, H, LAG, ME),
        grid=(n_pass, 4),
        in_specs=[full(a) for a in args],
        out_specs=pl.BlockSpec(memory_space=pl.ANY),
        out_shape=jax.ShapeDtypeStruct((N//R, R, R*C), BF16),
        scratch_shapes=[pltpu.VMEM((R, N, 2*C), BF16), pltpu.VMEM((R, 2*C, N), BF16), pltpu.VMEM((R, C, N), BF16),
                        pltpu.VMEM((R, C, N), F32), pltpu.VMEM((R, C, N), BF16), pltpu.VMEM((R, C, QB), BF16),
                        pltpu.VMEM((R*C, QB), BF16), pltpu.VMEM((R*C, QB), BF16), pltpu.VMEM((H, N, QB), F32),
                        pltpu.VMEM((N//R, R, R*C), BF16), pltpu.VMEM((2, N//R, R, R*C), BF16),
                        pltpu.VMEM((2, 4, TZ, TY, TX, TC, 2*H, R, 128), BF16),
                        pltpu.SemaphoreType.DMA, pltpu.SemaphoreType.DMA((2,)), pltpu.SemaphoreType.DMA,
                        pltpu.SemaphoreType.DMA((2, 4, 5)), pltpu.SemaphoreType.DMA((2, 4, 5))],
        compiler_params=pltpu.CompilerParams(dimension_semantics=("arbitrary", "arbitrary"), vmem_limit_bytes=60*2**20,
                                             collective_id=0, has_side_effects=True),
        cost_estimate=pl.CostEstimate(flops=flops, bytes_accessed=4*2**20, transcendentals=n_pass*R*H*N*N),
        name="mega",
    )(*args)


def prep_weights(ln_w, w_in, b_g, w_b, w_o, b_o, R):
    n, C, H = w_b.shape
    D = C // H
    lnw = jnp.swapaxes(ln_w.astype(F32), 1, 2)
    wt = jnp.swapaxes(w_in, 1, 2)
    wqvt = jnp.concatenate([wt[:, 0:C], wt[:, 2*C:4*C]], axis=1)
    wk = w_in[:, :, C:2*C].reshape(n, C, H, 1, D)
    wk2 = jnp.broadcast_to(wk, (n, C, H, 2, D)).reshape(n, C, 2*C)
    eye = jnp.eye(R, dtype=w_b.dtype)
    wbn = (jnp.swapaxes(w_b, 1, 2)[:, :, None, None, :] * eye[None, None, :, :, None]).reshape(n, H*R, R*C)
    col = lambda a: a.astype(F32)[:, :, None]
    return lnw, wqvt, wk2, col(b_g), jnp.swapaxes(w_o, 1, 2), col(b_o), wbn


def _ln_rows(x, w):
    x = x.astype(F32)
    mu = jnp.mean(x, axis=-1, keepdims=True)
    var = jnp.mean(jnp.square(x - mu), axis=-1, keepdims=True)
    y = (x - mu) * lax.rsqrt(var + EPS)
    return (y * w[0].astype(F32) + w[1].astype(F32)).astype(BF16)


def _rows(zl, bias, lw, wi, bg, wo, bo):
    h, n, _ = bias.shape
    c = zl.shape[-1]
    d = c // h

    def row(zr):
        y = _ln_rows(zr, lw)
        proj = jnp.transpose(jnp.dot(y, wi, preferred_element_type=F32).reshape(n, 4, h, d), (1, 2, 0, 3))
        gate = jax.nn.sigmoid(proj[3] + bg.astype(F32).reshape(h, 1, d))

        def head(a):
            q, k, v, b = a
            s = jnp.dot(q, k.T, preferred_element_type=F32) * d ** -0.5 + b
            return jnp.dot(jax.nn.softmax(s, axis=-1).astype(BF16), v, preferred_element_type=F32)

        o = lax.map(head, (*(a.astype(BF16) for a in proj[:3]), bias))
        o = jnp.transpose((gate * o).astype(BF16), (1, 0, 2)).reshape(n, c)
        return (zr.astype(F32) + jnp.dot(o, wo, preferred_element_type=F32) + bo.astype(F32)).astype(BF16)

    return lax.map(row, zl)


def _safe_to_skip_max(ws):
    ln_w, w_in, b_g, w_b, w_o, b_o = (a.astype(F32) for a in ws)
    n, C, H = w_b.shape
    D = C // H
    g, b = ln_w[:, 0], ln_w[:, 1]
    w = w_in.reshape(n, C, 4, H, D)[:, :, 0:3]
    wg = w * g[:, :, None, None, None]
    gram = jnp.sum(wg[..., :, None] * wg[..., None, :], axis=1)
    top = lambda m: jnp.sqrt(jnp.max(jnp.sum(jnp.abs(m), axis=-1), axis=-1) * C)
    both = top(jnp.sum(gram[:, 0, :, :, :, None] * gram[:, 1, :, None, :, :], axis=-2)) * C ** 0.5
    one = top(gram)
    off = jnp.sqrt(jnp.sum(jnp.square(jnp.sum(w * b[:, :, None, None, None], axis=1)), axis=-1))
    q, k, v = (one[:, a] + off[:, a] for a in range(3))
    qk = both + q * k - one[:, 0] * one[:, 1] + 0.02 * q * k
    nb = jnp.sqrt(jnp.sum(jnp.square(w_b * g[..., None]), axis=1) * C) + jnp.abs(jnp.sum(w_b * b[..., None], axis=1))
    return jnp.all((LOG2E * (qk * D ** -0.5 + 1.02 * nb) <= 100.0) & (v <= 2.0 ** 14))


def solution(mesh):
    def local(zl, res_mask, ln_w, w_in, b_g, w_b, w_o, b_o):
        R, N, C = zl.shape
        G = N // R
        mask_bias = jnp.where(res_mask > 0, 0.0, NEG).astype(F32)
        n = ln_w.shape[0] * ln_w.shape[1]
        ws = tuple(a.reshape(n, *a.shape[2:]) for a in (ln_w, w_in, b_g, w_b, w_o, b_o))

        def fast(zl):
            mask = jnp.broadcast_to(mask_bias[:, None], (N, 128))
            x = mega(jnp.swapaxes(zl, 1, 2), mask, *prep_weights(*ws, R))
            return jnp.transpose(x.reshape(G, R, R, C), (1, 0, 2, 3)).reshape(R, N, C)

        def exact(zl):
            def one(p, z):
                lw, wi, bg, wb, wo, bo = (lax.dynamic_index_in_dim(a, p, keepdims=False) for a in ws)
                b = jnp.dot(_ln_rows(z, lw).reshape(R*N, C), wb, preferred_element_type=F32).astype(BF16)
                b = lax.all_gather(b.reshape(R, N, -1), 'dap', axis=0, tiled=True)
                z = _rows(z, jnp.transpose(b, (2, 0, 1)).astype(F32) + mask_bias, lw, wi, bg, wo, bo)
                return jnp.swapaxes(lax.all_to_all(z, 'dap', 1, 0, tiled=True), 0, 1)
            return lax.fori_loop(0, n, one, zl)

        return lax.cond(_safe_to_skip_max(ws), fast, exact, zl)

    rows = P(('data', 'dap'))
    return jax.shard_map(local, mesh=mesh,
                         in_specs=(rows, P('data'), P(), P(), P(), P(), P(), P()),
                         out_specs=rows, check_vma=False)
```

```python
import functools
import jax
import jax.numpy as jnp
from jax import lax
from jax.experimental import pallas as pl
from jax.experimental.pallas import tpu as pltpu
from jax.sharding import PartitionSpec as P

F32 = jnp.float32
BF16 = jnp.bfloat16
EPS = 1e-5
NEG = -1e9
LOG2E = 1.4426950408889634
T = 4
BLOCKS = 4
PARTS = (((2, 1, 0), 0, 3), ((1, 0, 2), 3, 3), ((0, 2, 1), 6, 2))
MESH = pl.DeviceIdType.MESH
HIGH = lax.Precision.HIGHEST


def _ln_t(x, gamma, beta):
    mu = jnp.mean(x, axis=0, keepdims=True)
    d = x - mu
    var = jnp.mean(d*d, axis=0, keepdims=True)
    return (d * lax.rsqrt(var + EPS) * gamma + beta).astype(BF16)


def _place(b, r):
    z, y = r // (2*T), (r // 2) % T
    return z, y, (b + 2*T - z - y) % T, r % 2


def _index(z, y, x, c):
    return ((z*T + y)*T + x)*2 + c


def setup_kernel(R, ln_ref, win_ref, bg_ref, wbt_ref, wo_ref, bo_ref, m_ref,
                 cols_ref, wqvt_ref, wk2_ref, wot_ref, wbn_ref, mask_ref, ok_ref):
    n, H, C = wbt_ref.shape
    D = C // H
    iota = lambda shape, axis: lax.broadcasted_iota(jnp.int32, shape, axis)
    head = iota((C, C), 0) // D == iota((C, C), 1) // D
    lane = iota((C, 2*C), 1)
    twice = (iota((C, 2*C), 0) == (lane // (2*D)) * D + lane % D).astype(F32).astype(BF16)
    mine = iota((H, R, R*C), 1) == iota((H, R, R*C), 2) // C
    nt = lambda a, b: lax.dot_general(a, b, (((1,), (1,)), ((), ())), precision=HIGH, preferred_element_type=F32)
    whole = lambda f, a: f(f(a, axis=1, keepdims=True), axis=0, keepdims=True)
    top = lambda m: whole(lambda a, axis, keepdims: jnp.sum(a, axis=1, keepdims=True) if axis else
                          jnp.max(a, axis=0, keepdims=True), jnp.abs(m))
    good = jnp.ones((1, 1), F32)
    for p in range(n):
        ln = ln_ref[p].astype(F32)
        vecs = jnp.concatenate([ln, bg_ref[p:p+1].astype(F32), bo_ref[p:p+1].astype(F32), jnp.zeros((4, C), F32)], axis=0)
        cols_ref[p] = jnp.concatenate([vecs, jnp.zeros((8, C), F32)], axis=1).T[0:C]
        w = win_ref[p].T
        wqvt_ref[p, 0:C] = w[0:C]
        wqvt_ref[p, C:3*C] = w[2*C:4*C]
        wk = lax.dot_general(w[C:2*C], twice, (((0,), (0,)), ((), ())), preferred_element_type=F32)
        wk2_ref[p] = wk.astype(BF16)
        wot_ref[p] = wo_ref[p].T
        wb = wbt_ref[p].astype(F32)
        rep = jnp.concatenate([wb]*R, axis=1)
        wbn_ref[p] = jnp.where(mine, rep[:, None, :], 0.0).reshape(H*R, R*C).astype(BF16)

        w = w.astype(F32)
        wg = w * ln[0:1]
        gram = [jnp.where(head, nt(wg[a*C:(a+1)*C], wg[a*C:(a+1)*C]), 0.0) for a in range(3)]
        both = jnp.sqrt(top(jnp.dot(gram[0], gram[1], precision=HIGH, preferred_element_type=F32))) * C
        one = [jnp.sqrt(top(g) * C) for g in gram]
        off = jnp.square(jnp.sum(w * ln[1:2], axis=1, keepdims=True))
        per = lambda a: functools.reduce(jnp.maximum, [jnp.sum(off[a*C+h*D:a*C+(h+1)*D], axis=0, keepdims=True) for h in range(H)])
        q, k, v = (one[a] + jnp.sqrt(per(a)) for a in range(3))
        qk = both + q*k - one[0]*one[1] + 0.02*q*k
        nb = jnp.sqrt(jnp.sum(jnp.square(wb * ln[0:1]), axis=1, keepdims=True) * C) + jnp.abs(jnp.sum(wb * ln[1:2], axis=1, keepdims=True))
        s = LOG2E * (qk * D ** -0.5 + 1.02 * jnp.max(nb, axis=0, keepdims=True))
        good = jnp.where((s <= 100.0) & (v <= 2.0 ** 14), good, 0.0)
    ok_ref[0, 0] = jnp.min(good).astype(jnp.int32)

    cols = m_ref[...].astype(F32).T
    for j in range(m_ref.shape[0]):
        col = jnp.where(jnp.broadcast_to(cols[:, j:j+1], (128, 128)) > 0.0, 0.0, NEG)
        for e in range(8):
            g = 8*j + e
            z, y, x = g // (T*T), (g // T) % T, g % T
            to = (((z+y+x) % T)*2*T*T + (z*T+y)*2) * R
            mask_ref[to:to+2*R] = col[2*R*e:2*R*(e+1)]


def setup(ws, res_mask, R):
    n, C, H = ws[3].shape
    N = res_mask.shape[0]
    ln_w, w_in, b_g, w_b, w_o, b_o = ws
    sds = jax.ShapeDtypeStruct
    out = (sds((n, C, 8), F32), sds((n, 3*C, C), BF16), sds((n, C, 2*C), BF16), sds((n, C, C), BF16), sds((n, H*R, R*C), BF16),
           sds((N, 128), F32), sds((1, 1), jnp.int32))
    vmem, smem = pl.BlockSpec(memory_space=pltpu.VMEM), pl.BlockSpec(memory_space=pltpu.SMEM)
    return pl.pallas_call(functools.partial(setup_kernel, R), in_specs=[vmem]*7, out_specs=[vmem]*6 + [smem], out_shape=out,
                          name="setup")(ln_w, w_in, b_g, jnp.swapaxes(w_b, 1, 2), w_o, b_o, res_mask.reshape(N//128, 128))


def mega_kernel(R, N, C, H, LAG,
                z_ref, mask_ref, cols_ref, wqvt_ref, wk2_ref, wo_ref, wbn_ref,
                out_ref,
                k_s, q_s, v_s, g_s, z_s, o_s, y_s, zt_s, bias_s, x_s, r_s, G,
                a2a_send, a2a_recv, own_sem, ag_send, ag_recv):
    ps, jb = pl.program_id(0), pl.program_id(1)
    n_pass = cols_ref.shape[0]
    me = lax.axis_index('dap')
    n_dev = 2*T*T*T
    others = pl.ds(0, n_dev-1)
    D = C // H
    QB = N // BLOCKS
    KC = 128
    CH = N // KC
    DB = QB // R
    par, nxt = lax.rem(ps, 2), lax.rem(ps + 1, 2)
    q0 = pl.multiple_of(jb * QB, QB)
    core = me % 2
    at = (me // (2*T*T), (me // (2*T)) % T, (me // 2) % T)

    def moved(axis, by):
        p = list(at)
        p[axis] = (p[axis] + by) % T
        return p

    def copy(g, b, k, sel, u0, nu, to, c):
        r = G.at[g, b, sel[0], sel[1], sel[2], core, pl.ds(u0, nu)]
        return pltpu.make_async_remote_copy(r, r, ag_send.at[g, b, k], ag_recv.at[g, b, k],
                                            device_id={'dap': _index(*to, c)}, device_id_type=MESH)

    every = slice(None)
    sizes = ((0, pl.ds(0, 3), every), (pl.ds(0, 2), every, every), (0, every, every), (every,)*3, (0, 0, pl.ds(0, 3)))

    def landed(g, b, k, sem):
        for j in (k, 4) if k == 0 else (k,):
            r = G.at[(g, b) + sizes[j] + (0,)]
            pltpu.make_async_copy(r, r, sem.at[g, b, j]).wait()

    def stage(k, g, b):
        if k > 0:
            landed(g, b, k-1, ag_recv)
        if k == 4:
            for j in range(4):
                landed(g, b, j, ag_send)
            return
        if k == 3:
            r = G.at[g, b, :, :, :, core]
            pltpu.make_async_remote_copy(r, r, ag_send.at[g, b, 3], ag_recv.at[g, b, 3],
                                         device_id={'dap': _index(*at, 1-core)}, device_id_type=MESH).start()
            return
        for (a0, a1, a2), u0, nu in PARTS:
            if k == 0:
                def plane(e, sem):
                    to = list(at)
                    to[a0] = (at[a0] + e % T) % T
                    to[a1] = (at[a1] + e // T) % T
                    copy(g, b, sem, at, u0, nu, to, core).start()
                    return sem
                lax.fori_loop(1, T, plane, 4)
                lax.fori_loop(T, T*T, plane, 0)
                continue
            sel = list(at)
            sel[a0] = every
            for by, half in ((1, 0), (T-1, T//2)):
                if k == 1:
                    sel[a1] = every
                else:
                    sel[a1] = pl.ds(half, T//2)
                    sel[a2] = (at[a2] + T - by) % T
                copy(g, b, k, sel, u0, nu, moved(a2, by), core).start()

    def slot(s, p):
        for k in range(5):
            b = s - k
            if isinstance(s, int):
                if 0 <= b < BLOCKS:
                    stage(k, (p + 1) % 2, b)
                continue
            if k < BLOCKS:
                @pl.when((b >= 0) & (p < n_pass-1))
                def _():
                    stage(k, (p + 1) % 2, b)
            if k > 1:
                @pl.when((b < 0) & (b + 5 < BLOCKS) & (p >= 1))
                def _():
                    stage(k, p % 2, b + 5)

    def put_bias(g, b, rows):
        for h in range(H):
            for t in range(2):
                G[g, b, at[0], at[1], at[2], core, 2*h+t] = rows[h*R:(h+1)*R, t*128:(t+1)*128]

    def col(p, j):
        return cols_ref[p, :, j:j+1]

    def bias_rows(p, y):
        return jnp.dot(wbn_ref[p], y, preferred_element_type=F32).astype(BF16)

    def prep(i):
        y = _ln_t(z_s[i].astype(F32), col(ps, 0), col(ps, 1))
        p = jnp.dot(wqvt_ref[ps], y, preferred_element_type=F32)
        k_s[i] = jnp.dot(y.T, wk2_ref[ps], preferred_element_type=F32).astype(BF16)
        q = p[0:C].astype(BF16).astype(F32) * (LOG2E * D ** -0.5)
        qh = q.astype(BF16)
        ql = (q - qh.astype(F32)).astype(BF16)
        for h in range(H):
            q_s[i, 2*D*h:2*D*h+D] = qh[D*h:D*h+D]
            q_s[i, 2*D*h+D:2*D*h+2*D] = ql[D*h:D*h+D]
        v_s[i] = p[C:2*C].astype(BF16)
        g_s[i] = jax.nn.sigmoid(p[2*C:3*C] + col(ps, 2))

    def prep_all():
        def two(t, _):
            prep(2*t)
            prep(2*t+1)
            return 0
        lax.fori_loop(0, R//2, two, 0)

    def unpack(g, w, by_place):
        src = [16*w + k for k in range(16)]
        if by_place:
            src = [_index(*_place(w // 2, (w % 2)*16 + k)) for k in range(16)]
        t = jnp.concatenate([r_s[g, s] for s in src], axis=0).astype(F32).T
        x = [t[i*C:(i+1)*C] for i in range(R)]
        lane = lax.broadcasted_iota(jnp.int32, (C, 128), 1)
        for bit in (1, 2, 4):
            odd = (lane & bit) != 0
            for i in range(R):
                if not i & bit:
                    a, b = x[i], x[i | bit]
                    x[i] = jnp.where(odd, pltpu.roll(b, bit, 1), a)
                    x[i | bit] = jnp.where(odd, b, pltpu.roll(a, 128-bit, 1))
        for i in range(R):
            z_s[i, :, pl.ds(pl.multiple_of(w*128, 128), 128)] = x[i].astype(BF16)

    def arrived(g, by_place):
        pltpu.make_async_copy(r_s.at[g, others], r_s.at[g, others], a2a_recv.at[g]).wait()
        pltpu.make_async_copy(r_s.at[g, others], r_s.at[g, others], a2a_send).wait()
        def two(t, _):
            unpack(g, 2*t, by_place)
            unpack(g, 2*t+1, by_place)
            return 0
        lax.fori_loop(0, N//256, two, 0)

    @pl.when((jb == 0) & (ps == 0))
    def _():
        barrier = pltpu.get_barrier_semaphore()
        def greet(k, _):
            pl.semaphore_signal(barrier, inc=1, device_id={'dap': (me + k) % n_dev}, device_id_type=MESH)
            return 0
        lax.fori_loop(1, n_dev, greet, 0)
        def first(b, _):
            row = lax.broadcasted_iota(jnp.int32, (N, QB), 0)
            lane = lax.broadcasted_iota(jnp.int32, (N, QB), 1)
            r = lane // R
            z, y = r // (2*T), (r // 2) % T
            x = (b + 2*T - z - y) % T
            turn = (row == (((z*T + y)*T + x)*2 + r % 2)*R + lane % R).astype(F32).astype(BF16)
            qs = pl.ds(pl.multiple_of(b*QB, QB), QB)
            for i in range(R):
                zb = jnp.dot(z_ref[i], turn, preferred_element_type=F32)
                z_s[i, :, qs] = zb.astype(BF16)
                y_s[i*C:(i+1)*C] = _ln_t(zb, col(0, 0), col(0, 1))
            put_bias(0, b, bias_rows(0, y_s[...]))
            return 0
        lax.fori_loop(0, BLOCKS, first, 0)
        pl.semaphore_wait(barrier, n_dev - 1)
        def gather(k):
            def each(b, _):
                stage(k, 0, b)
                return 0
            lax.fori_loop(0, BLOCKS, each, 0)
        gather(0)
        gather(1)
        prep_all()
        gather(2)
        gather(3)
        gather(4)

    @pl.when((jb == 0) & (ps > 0))
    def _():
        arrived(par, True)
        prep_all()
        slot(4, ps-1)

    @pl.when(ps == 0)
    def _():
        def each(h, _):
            for b in range(BLOCKS):
                for t in range(2):
                    v = [G[(0, b) + _place(jb, r) + (2*h+t,)] for r in range(DB)]
                    v = jnp.concatenate(v, axis=0).astype(F32).T * LOG2E
                    rows = slice((2*b+t)*128, (2*b+t+1)*128)
                    for w in range(2):
                        bias_s[h, rows, w*128:(w+1)*128] = v[:, w*128:(w+1)*128] + mask_ref[rows]
            return 0
        lax.fori_loop(0, H, each, 0)

    @pl.when(ps > 0)
    def _():
        def each(h, _):
            for m in range(CH):
                for w in range(2):
                    v = [G[(par, jb) + _place(m // 2, (m % 2)*16 + r) + (2*h+w,)] for r in range(16)]
                    v = jnp.concatenate(v, axis=0).astype(F32)
                    bias_s[h, m*128:(m+1)*128, w*128:(w+1)*128] = v * LOG2E + mask_ref[m*128:(m+1)*128]
            return 0
        lax.fori_loop(0, H, each, 0)

    zl = jnp.zeros((KC, 256-2*C), BF16)
    zp = jnp.zeros((KC, QB), BF16)
    zv = jnp.zeros((D, 256-KC), BF16)
    zq = jnp.zeros((2*D, QB), BF16)
    steps = [(h, c) for h in range(H) for c in range(CH)]
    S = len(steps)
    es, ss, acc, tot = {}, {}, [None]*R, [None]*R
    for n in range(-LAG, S):
        if n >= 0:
            h, c = steps[n]
            b = bias_s[h, c*KC:(c+1)*KC]
            for i in range(R):
                e = jnp.exp2(ss.pop((n, i)) + b)
                es[i] = e.astype(BF16)
                e = jnp.sum(e.reshape(KC//8, 8, QB), axis=0)
                tot[i] = e if c == 0 else tot[i] + e
        for i in range(R):
            rows = []
            w = zp
            if n+LAG < S:
                h2, c2 = steps[n+LAG]
                w = jnp.concatenate([zq]*h2 + [q_s[i, 2*D*h2:2*D*(h2+1), pl.ds(q0, QB)]] + [zq]*(H-1-h2), axis=0)
                rows.append(jnp.concatenate([zl, k_s[i, c2*KC:(c2+1)*KC]], axis=1))
            if n >= 0:
                rows.append(jnp.concatenate([v_s[i, D*h:D*h+D, c*KC:(c+1)*KC], zv], axis=1))
            o = jnp.dot(jnp.concatenate(rows, axis=0), jnp.concatenate([es.pop(i) if n >= 0 else zp, w], axis=0),
                        preferred_element_type=F32)
            if n+LAG < S:
                ss[n+LAG, i] = o[0:KC]
            if n >= 0:
                o = o[-D:]
                acc[i] = o if c == 0 else acc[i] + o
                if c == CH-1:
                    a = acc[i] / jnp.sum(tot[i], axis=0, keepdims=True)
                    o_s[i, D*h:D*h+D] = (g_s[i, D*h:D*h+D, pl.ds(q0, QB)] * a).astype(BF16)

    pn = (ps + 1) % n_pass

    def upd(t, _):
        for j in range(4):
            i = 4*t + j
            u = jnp.dot(wo_ref[ps], o_s[i], preferred_element_type=F32) + col(ps, 3)
            zn = (z_s[i, :, pl.ds(q0, QB)].astype(F32) + u).astype(BF16)
            rows = pl.ds(pl.multiple_of(i*C, C), C)
            zt_s[rows] = zn
            y_s[rows] = _ln_t(zn.astype(F32), col(pn, 0), col(pn, 1))
        return 0
    lax.fori_loop(0, R//4, upd, 0)
    x_s[pl.ds(jb*DB, DB)] = zt_s[...].T.reshape(DB, R, R*C)

    @pl.when(ps < n_pass-1)
    def _():
        put_bias(nxt, jb, bias_rows(pn, y_s[...]))

    def send(k, _):
        d = _index(*_place(jb, k))
        @pl.when(d != me)
        def _():
            pltpu.make_async_remote_copy(x_s.at[jb*DB + k], r_s.at[nxt, me], a2a_send, a2a_recv.at[nxt],
                                         device_id={'dap': d}, device_id_type=MESH).start()
        return 0
    lax.fori_loop(0, DB, send, 0)

    @pl.when((at[0] + at[1] + at[2]) % T == jb)
    def _():
        r_s[nxt, me] = x_s[jb*DB + (at[0]*T + at[1])*2 + core]
    slot(jb, ps)

    @pl.when((ps == n_pass-1) & (jb == BLOCKS-1))
    def _():
        arrived(nxt, False)
        out = pltpu.make_async_copy(z_s, out_ref, own_sem)
        out.start()
        out.wait()


def mega(z, mask, cols, wqvt, wk2, wo, wbn, LAG=2):
    R, C, N = z.shape
    n_pass = cols.shape[0]
    H = wbn.shape[1] // R
    QB = N // BLOCKS
    full = lambda a: pl.BlockSpec(a.shape, lambda p, j: (0,)*a.ndim, pipeline_mode=pl.Buffered(1))
    args = (z, mask, cols, wqvt, wk2, wo, wbn)
    dma = pltpu.SemaphoreType.DMA
    return pl.pallas_call(
        functools.partial(mega_kernel, R, N, C, H, LAG),
        grid=(n_pass, BLOCKS),
        in_specs=[full(a) for a in args],
        out_specs=pl.BlockSpec(memory_space=pl.ANY),
        out_shape=jax.ShapeDtypeStruct((R, C, N), BF16),
        scratch_shapes=[pltpu.VMEM((R, N, 2*C), BF16), pltpu.VMEM((R, 2*C, N), BF16), pltpu.VMEM((R, C, N), BF16),
                        pltpu.VMEM((R, C, N), F32), pltpu.VMEM((R, C, N), BF16), pltpu.VMEM((R, C, QB), BF16),
                        pltpu.VMEM((R*C, QB), BF16), pltpu.VMEM((R*C, QB), BF16), pltpu.VMEM((H, N, QB), F32),
                        pltpu.VMEM((N//R, R, R*C), BF16), pltpu.VMEM((2, N//R, R, R*C), BF16),
                        pltpu.VMEM((2, BLOCKS, T, T, T, 2, 2*H, R, 128), BF16),
                        dma, dma((2,)), dma, dma((2, BLOCKS, 5)), dma((2, BLOCKS, 5))],
        compiler_params=pltpu.CompilerParams(dimension_semantics=("arbitrary", "arbitrary"), vmem_limit_bytes=60*2**20,
                                             collective_id=0, has_side_effects=True),
        cost_estimate=pl.CostEstimate(flops=n_pass*4*R*H*N*N*(C//H), bytes_accessed=4*N*R*C, transcendentals=n_pass*R*H*N*N),
        name="mega",
    )(*args)


def _ln_rows(x, w):
    x = x.astype(F32)
    mu = jnp.mean(x, axis=-1, keepdims=True)
    var = jnp.mean(jnp.square(x - mu), axis=-1, keepdims=True)
    y = (x - mu) * lax.rsqrt(var + EPS)
    return (y * w[0].astype(F32) + w[1].astype(F32)).astype(BF16)


def _rows(zl, bias, lw, wi, bg, wo, bo):
    h, n, _ = bias.shape
    c = zl.shape[-1]
    d = c // h

    def row(zr):
        y = _ln_rows(zr, lw)
        proj = jnp.transpose(jnp.dot(y, wi, preferred_element_type=F32).reshape(n, 4, h, d), (1, 2, 0, 3))
        gate = jax.nn.sigmoid(proj[3] + bg.astype(F32).reshape(h, 1, d))

        def head(a):
            q, k, v, b = a
            s = jnp.dot(q, k.T, preferred_element_type=F32) * d ** -0.5 + b
            return jnp.dot(jax.nn.softmax(s, axis=-1).astype(BF16), v, preferred_element_type=F32)

        o = lax.map(head, (*(a.astype(BF16) for a in proj[:3]), bias))
        o = jnp.transpose((gate * o).astype(BF16), (1, 0, 2)).reshape(n, c)
        return (zr.astype(F32) + jnp.dot(o, wo, preferred_element_type=F32) + bo.astype(F32)).astype(BF16)

    return lax.map(row, zl)


def solution(mesh):
    def local(zl, res_mask, ln_w, w_in, b_g, w_b, w_o, b_o):
        R, N, C = zl.shape
        n = ln_w.shape[0] * ln_w.shape[1]
        ws = tuple(a.reshape(n, *a.shape[2:]) for a in (ln_w, w_in, b_g, w_b, w_o, b_o))
        cols, wqvt, wk2, wo, wbn, mask, ok = setup(ws, res_mask, R)

        def fast(zl):
            return jnp.swapaxes(mega(jnp.swapaxes(zl, 1, 2), mask, cols, wqvt, wk2, wo, wbn), 1, 2)

        def exact(zl):
            mask_bias = jnp.where(res_mask > 0, 0.0, NEG).astype(F32)

            def one(p, z):
                lw, wi, bg, wb, wo, bo = (lax.dynamic_index_in_dim(a, p, keepdims=False) for a in ws)
                b = jnp.dot(_ln_rows(z, lw).reshape(R*N, C), wb, preferred_element_type=F32).astype(BF16)
                b = jnp.transpose(b.reshape(R, 8, N//8, -1), (3, 1, 0, 2))
                b = b.reshape(-1, R, N//8)
                bias = lax.map(lambda a: lax.all_gather(a, 'dap', axis=0, tiled=True), b)
                bias = jnp.swapaxes(bias.reshape(-1, 8, N, N//8), 1, 2).reshape(-1, N, N)
                z = _rows(z, bias.astype(F32) + mask_bias, lw, wi, bg, wo, bo)
                return jnp.swapaxes(lax.all_to_all(z, 'dap', 1, 0, tiled=True), 0, 1)
            return lax.fori_loop(0, n, one, zl)

        return lax.cond(ok[0, 0] > 0, fast, exact, zl)

    rows = P(('data', 'dap'))
    return jax.shard_map(local, mesh=mesh,
                         in_specs=(rows, P('data'), P(), P(), P(), P(), P(), P()),
                         out_specs=rows, check_vma=False)
```

```python
import functools
import jax
import jax.numpy as jnp
from jax import lax
from jax.experimental import pallas as pl
from jax.experimental.pallas import tpu as pltpu
from jax.sharding import PartitionSpec as P

F32 = jnp.float32
BF16 = jnp.bfloat16
EPS = 1e-5
NEG = -1e9
LOG2E = 1.4426950408889634
T = 4
BLOCKS = 4
PARTS = (((2, 1, 0), 0, 3), ((1, 0, 2), 3, 3), ((0, 2, 1), 6, 2))
MESH = pl.DeviceIdType.MESH
HIGH = lax.Precision.HIGHEST


def _ln_t(x, gamma, beta):
    mu = jnp.mean(x, axis=0, keepdims=True)
    d = x - mu
    var = jnp.mean(d*d, axis=0, keepdims=True)
    return (d * lax.rsqrt(var + EPS) * gamma + beta).astype(BF16)


def _place(b, r):
    z, y = r // (2*T), (r // 2) % T
    return z, y, 2*(r % 2) + (b // 2 + z + y) % 2, b % 2


def _block(z, y, x, c):
    return (z + y + x) % 2 * 2 + c, (z*T + y)*2 + x // 2


def _index(z, y, x, c):
    return ((z*T + y)*T + x)*2 + c


def setup_kernel(R, ln_ref, win_ref, bg_ref, wbt_ref, wo_ref, bo_ref, m_ref,
                 cols_ref, wqvt_ref, wk2_ref, wot_ref, wbn_ref, mask_ref, ok_ref):
    n, H, C = wbt_ref.shape
    D = C // H
    iota = lambda shape, axis: lax.broadcasted_iota(jnp.int32, shape, axis)
    head = iota((C, C), 0) // D == iota((C, C), 1) // D
    lane = iota((C, 2*C), 1)
    twice = (iota((C, 2*C), 0) == (lane // (2*D)) * D + lane % D).astype(F32).astype(BF16)
    mine = iota((H, R, R*C), 1) == iota((H, R, R*C), 2) // C
    nt = lambda a, b: lax.dot_general(a, b, (((1,), (1,)), ((), ())), precision=HIGH, preferred_element_type=F32)
    whole = lambda f, a: f(f(a, axis=1, keepdims=True), axis=0, keepdims=True)
    top = lambda m: whole(lambda a, axis, keepdims: jnp.sum(a, axis=1, keepdims=True) if axis else
                          jnp.max(a, axis=0, keepdims=True), jnp.abs(m))
    good = jnp.ones((1, 1), F32)
    for p in range(n):
        ln = ln_ref[p].astype(F32)
        vecs = jnp.concatenate([ln, bg_ref[p:p+1].astype(F32), bo_ref[p:p+1].astype(F32), jnp.zeros((4, C), F32)], axis=0)
        cols_ref[p] = jnp.concatenate([vecs, jnp.zeros((8, C), F32)], axis=1).T[0:C]
        w = win_ref[p].T
        wqvt_ref[p, 0:C] = w[0:C]
        wqvt_ref[p, C:3*C] = w[2*C:4*C]
        wk = lax.dot_general(w[C:2*C], twice, (((0,), (0,)), ((), ())), preferred_element_type=F32)
        wk2_ref[p] = wk.astype(BF16)
        wot_ref[p] = wo_ref[p].T
        wb = wbt_ref[p].astype(F32)
        rep = jnp.concatenate([wb]*R, axis=1)
        wbn_ref[p] = jnp.where(mine, rep[:, None, :], 0.0).reshape(H*R, R*C).astype(BF16)

        w = w.astype(F32)
        wg = w * ln[0:1]
        gram = [jnp.where(head, nt(wg[a*C:(a+1)*C], wg[a*C:(a+1)*C]), 0.0) for a in range(3)]
        both = jnp.sqrt(top(jnp.dot(gram[0], gram[1], precision=HIGH, preferred_element_type=F32))) * C
        one = [jnp.sqrt(top(g) * C) for g in gram]
        off = jnp.square(jnp.sum(w * ln[1:2], axis=1, keepdims=True))
        per = lambda a: functools.reduce(jnp.maximum, [jnp.sum(off[a*C+h*D:a*C+(h+1)*D], axis=0, keepdims=True) for h in range(H)])
        q, k, v = (one[a] + jnp.sqrt(per(a)) for a in range(3))
        qk = both + q*k - one[0]*one[1] + 0.02*q*k
        nb = jnp.sqrt(jnp.sum(jnp.square(wb * ln[0:1]), axis=1, keepdims=True) * C) + jnp.abs(jnp.sum(wb * ln[1:2], axis=1, keepdims=True))
        s = LOG2E * (qk * D ** -0.5 + 1.02 * jnp.max(nb, axis=0, keepdims=True))
        good = jnp.where((s <= 100.0) & (v <= 2.0 ** 14), good, 0.0)
    ok_ref[0, 0] = jnp.min(good).astype(jnp.int32)

    cols = m_ref[...].astype(F32).T
    for j in range(m_ref.shape[0]):
        col = jnp.where(jnp.broadcast_to(cols[:, j:j+1], (128, 128)) > 0.0, 0.0, NEG)
        for e in range(16):
            g = 16*j + e
            b, r = _block(g // (2*T*T), (g // (2*T)) % T, (g // 2) % T, g % 2)
            mask_ref[(b*2*T*T + r)*R:(b*2*T*T + r + 1)*R] = col[R*e:R*(e+1)]


def setup(ws, res_mask, R):
    n, C, H = ws[3].shape
    N = res_mask.shape[0]
    ln_w, w_in, b_g, w_b, w_o, b_o = ws
    sds = jax.ShapeDtypeStruct
    out = (sds((n, C, 8), F32), sds((n, 3*C, C), BF16), sds((n, C, 2*C), BF16), sds((n, C, C), BF16), sds((n, H*R, R*C), BF16),
           sds((N, 128), F32), sds((1, 1), jnp.int32))
    vmem, smem = pl.BlockSpec(memory_space=pltpu.VMEM), pl.BlockSpec(memory_space=pltpu.SMEM)
    return pl.pallas_call(functools.partial(setup_kernel, R), in_specs=[vmem]*7, out_specs=[vmem]*6 + [smem], out_shape=out,
                          name="setup")(ln_w, w_in, b_g, jnp.swapaxes(w_b, 1, 2), w_o, b_o, res_mask.reshape(N//128, 128))


def mega_kernel(R, N, C, H, LAG,
                z_ref, mask_ref, cols_ref, wqvt_ref, wk2_ref, wo_ref, wbn_ref,
                out_ref,
                k_s, q_s, v_s, g_s, z_s, o_s, y_s, zt_s, bias_s, x_s, r_s, G,
                a2a_send, a2a_recv, own_sem, ag_send, ag_recv):
    ps, jb = pl.program_id(0), pl.program_id(1)
    n_pass = cols_ref.shape[0]
    me = lax.axis_index('dap')
    n_dev = 2*T*T*T
    others = pl.ds(0, n_dev-1)
    D = C // H
    QB = N // BLOCKS
    KC = 128
    CH = N // KC
    DB = QB // R
    par, nxt = lax.rem(ps, 2), lax.rem(ps + 1, 2)
    q0 = pl.multiple_of(jb * QB, QB)
    core = me % 2
    at = (me // (2*T*T), (me // (2*T)) % T, (me // 2) % T)
    my_block, my_place = _block(*at, core)
    last = ps // (n_pass-1)
    slot_of_me = (my_block*DB + my_place) * (1-last) + me * last

    def moved(axis, by):
        p = list(at)
        p[axis] = (p[axis] + by) % T
        return p

    def copy(g, b, k, sel, u0, nu, to, c):
        r = G.at[g, b, sel[0], sel[1], sel[2], core, pl.ds(u0, nu)]
        return pltpu.make_async_remote_copy(r, r, ag_send.at[g, b, k], ag_recv.at[g, b, k],
                                            device_id={'dap': _index(*to, c)}, device_id_type=MESH)

    every = slice(None)
    sizes = ((0, pl.ds(0, 3), every), (pl.ds(0, 2), every, every), (0, every, every), (every,)*3, (0, 0, pl.ds(0, 3)))

    def landed(g, b, k, sem):
        for j in (k, 4) if k == 0 else (k,):
            r = G.at[(g, b) + sizes[j] + (0,)]
            pltpu.make_async_copy(r, r, sem.at[g, b, j]).wait()

    def stage(k, g, b):
        if k > 0:
            landed(g, b, k-1, ag_recv)
        if k == 4:
            for j in range(4):
                landed(g, b, j, ag_send)
            return
        if k == 3:
            r = G.at[g, b, :, :, :, core]
            pltpu.make_async_remote_copy(r, r, ag_send.at[g, b, 3], ag_recv.at[g, b, 3],
                                         device_id={'dap': _index(*at, 1-core)}, device_id_type=MESH).start()
            return
        for (a0, a1, a2), u0, nu in PARTS:
            if k == 0:
                def plane(e, sem):
                    to = moved(a0, e % T)
                    to[a1] = (at[a1] + e // T) % T
                    copy(g, b, sem, at, u0, nu, to, core).start()
                    return sem
                lax.fori_loop(1, T, plane, 4)
                lax.fori_loop(T, T*T, plane, 0)
                continue
            sel = list(at)
            sel[a0] = every
            for by, half in ((1, 0), (T-1, T//2)):
                if k == 1:
                    sel[a1] = every
                else:
                    sel[a1] = pl.ds(half, T//2)
                    sel[a2] = (at[a2] + T - by) % T
                copy(g, b, k, sel, u0, nu, moved(a2, by), core).start()

    def slot(s, p):
        for k in range(5):
            b = s - k
            if isinstance(s, int):
                if 0 < b < BLOCKS:
                    stage(k, (p + 1) % 2, b)
                continue
            if k < BLOCKS:
                @pl.when((b >= 0) & (p < n_pass-1))
                def _():
                    stage(k, (p + 1) % 2, b)
            if k > 1:
                @pl.when((b < 0) & (b + 5 < BLOCKS) & (p >= 1))
                def _():
                    stage(k, p % 2, b + 5)

    def put_bias(g, b, rows):
        for h in range(H):
            for t in range(2):
                G[g, b, at[0], at[1], at[2], core, 2*h+t] = rows[h*R:(h+1)*R, t*128:(t+1)*128]

    def col(p, j):
        return cols_ref[p, :, j:j+1]

    def bias_rows(p, y):
        return jnp.dot(wbn_ref[p], y, preferred_element_type=F32).astype(BF16)

    def prep(i):
        y = _ln_t(z_s[i].astype(F32), col(ps, 0), col(ps, 1))
        p = jnp.dot(wqvt_ref[ps], y, preferred_element_type=F32)
        k_s[i] = jnp.dot(y.T, wk2_ref[ps], preferred_element_type=F32).astype(BF16)
        q = p[0:C].astype(BF16).astype(F32) * (LOG2E * D ** -0.5)
        qh = q.astype(BF16)
        ql = (q - qh.astype(F32)).astype(BF16)
        for h in range(H):
            q_s[i, 2*D*h:2*D*h+D] = qh[D*h:D*h+D]
            q_s[i, 2*D*h+D:2*D*h+2*D] = ql[D*h:D*h+D]
        v_s[i] = p[C:2*C].astype(BF16)
        g_s[i] = jax.nn.sigmoid(p[2*C:3*C] + col(ps, 2))

    def prep_all():
        def two(t, _):
            prep(2*t)
            prep(2*t+1)
            return 0
        lax.fori_loop(0, R//2, two, 0)

    def unpack(g, w):
        t = r_s[g, pl.ds(w*16, 16)].reshape(16*R, R*C).astype(F32).T
        x = [t[i*C:(i+1)*C] for i in range(R)]
        lane = lax.broadcasted_iota(jnp.int32, (C, 128), 1)
        for bit in (1, 2, 4):
            odd = (lane & bit) != 0
            for i in range(R):
                if not i & bit:
                    a, b = x[i], x[i | bit]
                    x[i] = jnp.where(odd, pltpu.roll(b, bit, 1), a)
                    x[i | bit] = jnp.where(odd, b, pltpu.roll(a, 128-bit, 1))
        for i in range(R):
            z_s[i, :, pl.ds(pl.multiple_of(w*128, 128), 128)] = x[i].astype(BF16)

    def arrived(g):
        pltpu.make_async_copy(r_s.at[g, others], r_s.at[g, others], a2a_recv.at[g]).wait()
        pltpu.make_async_copy(r_s.at[g, others], r_s.at[g, others], a2a_send).wait()
        def two(t, _):
            unpack(g, 2*t)
            unpack(g, 2*t+1)
            return 0
        lax.fori_loop(0, N//256, two, 0)

    def to_f32(b, h, m):
        for w in range(2):
            v = [G[(par, b) + _place(m // 2, (m % 2)*16 + r) + (2*h+w,)] for r in range(16)]
            v = jnp.concatenate(v, axis=0).astype(F32)
            bias_s[h, m*128:(m+1)*128, w*128:(w+1)*128] = v * LOG2E + mask_ref[m*128:(m+1)*128]

    def to_f32_all(b):
        def each(h, _):
            for m in range(CH):
                to_f32(b, h, m)
            return 0
        lax.fori_loop(0, H, each, 0)

    def turn_bias(h, _):
        for b in range(BLOCKS):
            for a in range(b+1):
                got = {}
                for u, v in ((a, b), (b, a))[a == b:]:
                    for t in range(2):
                        x = [G[(0, u) + _place(v, r) + (2*h+t,)] for r in range(DB)]
                        got[u, v, t] = jnp.concatenate(x, axis=0).astype(F32).T.astype(BF16)
                for (u, v, t), x in got.items():
                    for r in range(16):
                        for w in range(2):
                            G[(0, v) + _place(u, t*16 + r) + (2*h+w,)] = x[r*R:(r+1)*R, w*128:(w+1)*128]
        return 0

    @pl.when((jb == 0) & (ps == 0))
    def _():
        barrier = pltpu.get_barrier_semaphore()
        def greet(k, _):
            pl.semaphore_signal(barrier, inc=1, device_id={'dap': (me + k) % n_dev}, device_id_type=MESH)
            return 0
        lax.fori_loop(1, n_dev, greet, 0)
        def first(b, _):
            row = lax.broadcasted_iota(jnp.int32, (N, QB), 0)
            lane = lax.broadcasted_iota(jnp.int32, (N, QB), 1)
            r = lane // R
            turn = (row == _index(*_place(b, r))*R + lane % R).astype(F32).astype(BF16)
            qs = pl.ds(pl.multiple_of(b*QB, QB), QB)
            for i in range(R):
                zb = jnp.dot(z_ref[i], turn, preferred_element_type=F32)
                z_s[i, :, qs] = zb.astype(BF16)
                y_s[i*C:(i+1)*C] = _ln_t(zb, col(0, 0), col(0, 1))
            put_bias(0, b, bias_rows(0, y_s[...]))
            return 0
        lax.fori_loop(0, BLOCKS, first, 0)
        pl.semaphore_wait(barrier, n_dev - 1)
        def gather(k):
            def each(b, _):
                stage(k, 0, b)
                return 0
            lax.fori_loop(0, BLOCKS, each, 0)
        gather(0)
        gather(1)
        prep_all()
        gather(2)
        gather(3)
        gather(4)
        lax.fori_loop(0, H, turn_bias, 0)
        to_f32_all(0)

    @pl.when((jb == 0) & (ps > 0))
    def _():
        stage(4, par, 0)
        to_f32_all(0)
        arrived(par)
        prep_all()
        slot(4, ps-1)

    @pl.when(jb > 0)
    def _():
        to_f32_all(jb)

    zl = jnp.zeros((KC, 256-2*C), BF16)
    zp = jnp.zeros((KC, QB), BF16)
    zv = jnp.zeros((D, 256-KC), BF16)
    zq = jnp.zeros((2*D, QB), BF16)
    steps = [(h, c) for h in range(H) for c in range(CH)]
    S = len(steps)
    es, ss, acc, tot = {}, {}, [None]*R, [None]*R
    for n in range(-LAG, S):
        if n >= 0:
            h, c = steps[n]
            b = bias_s[h, c*KC:(c+1)*KC]
            for i in range(R):
                e = jnp.exp2(ss.pop((n, i)) + b)
                es[i] = e.astype(BF16)
                e = jnp.sum(e.reshape(KC//8, 8, QB), axis=0)
                tot[i] = e if c == 0 else tot[i] + e
        for i in range(R):
            rows = []
            w = zp
            if n+LAG < S:
                h2, c2 = steps[n+LAG]
                w = jnp.concatenate([zq]*h2 + [q_s[i, 2*D*h2:2*D*(h2+1), pl.ds(q0, QB)]] + [zq]*(H-1-h2), axis=0)
                rows.append(jnp.concatenate([zl, k_s[i, c2*KC:(c2+1)*KC]], axis=1))
            if n >= 0:
                rows.append(jnp.concatenate([v_s[i, D*h:D*h+D, c*KC:(c+1)*KC], zv], axis=1))
            o = jnp.dot(jnp.concatenate(rows, axis=0), jnp.concatenate([es.pop(i) if n >= 0 else zp, w], axis=0),
                        preferred_element_type=F32)
            if n+LAG < S:
                ss[n+LAG, i] = o[0:KC]
            if n >= 0:
                o = o[-D:]
                acc[i] = o if c == 0 else acc[i] + o
                if c == CH-1:
                    a = acc[i] / jnp.sum(tot[i], axis=0, keepdims=True)
                    o_s[i, D*h:D*h+D] = (g_s[i, D*h:D*h+D, pl.ds(q0, QB)] * a).astype(BF16)

    def upd(t, _):
        for j in range(4):
            i = 4*t + j
            u = jnp.dot(wo_ref[ps], o_s[i], preferred_element_type=F32) + col(ps, 3)
            zt_s[pl.ds(pl.multiple_of(i*C, C), C)] = (z_s[i, :, pl.ds(q0, QB)].astype(F32) + u).astype(BF16)
        return 0
    lax.fori_loop(0, R//4, upd, 0)
    x_s[pl.ds(jb*DB, DB)] = zt_s[...].T.reshape(DB, R, R*C)

    def send(t, _):
        for j in range(4):
            k = 4*t + j
            d = _index(*_place(jb, k))
            @pl.when(d != me)
            def _():
                pltpu.make_async_remote_copy(x_s.at[jb*DB + k], r_s.at[nxt, slot_of_me], a2a_send, a2a_recv.at[nxt],
                                             device_id={'dap': d}, device_id_type=MESH).start()
        return 0
    lax.fori_loop(0, DB//4, send, 0)

    @pl.when(my_block == jb)
    def _():
        r_s[nxt, slot_of_me] = x_s[jb*DB + my_place]

    @pl.when(ps < n_pass-1)
    def _():
        def norm(t, _):
            for j in range(4):
                rows = pl.ds(pl.multiple_of((4*t + j)*C, C), C)
                y_s[rows] = _ln_t(zt_s[rows].astype(F32), col(ps+1, 0), col(ps+1, 1))
            return 0
        lax.fori_loop(0, R//4, norm, 0)
        put_bias(nxt, jb, bias_rows(ps+1, y_s[...]))
    slot(jb, ps)

    @pl.when((ps == n_pass-1) & (jb == BLOCKS-1))
    def _():
        arrived(nxt)
        out = pltpu.make_async_copy(z_s, out_ref, own_sem)
        out.start()
        out.wait()


def mega(z, mask, cols, wqvt, wk2, wo, wbn, LAG=2):
    R, C, N = z.shape
    n_pass = cols.shape[0]
    H = wbn.shape[1] // R
    QB = N // BLOCKS
    full = lambda a: pl.BlockSpec(a.shape, lambda p, j: (0,)*a.ndim, pipeline_mode=pl.Buffered(1))
    args = (z, mask, cols, wqvt, wk2, wo, wbn)
    dma = pltpu.SemaphoreType.DMA
    return pl.pallas_call(
        functools.partial(mega_kernel, R, N, C, H, LAG),
        grid=(n_pass, BLOCKS),
        in_specs=[full(a) for a in args],
        out_specs=pl.BlockSpec(memory_space=pl.ANY),
        out_shape=jax.ShapeDtypeStruct((R, C, N), BF16),
        scratch_shapes=[pltpu.VMEM((R, N, 2*C), BF16), pltpu.VMEM((R, 2*C, N), BF16), pltpu.VMEM((R, C, N), BF16),
                        pltpu.VMEM((R, C, N), F32), pltpu.VMEM((R, C, N), BF16), pltpu.VMEM((R, C, QB), BF16),
                        pltpu.VMEM((R*C, QB), BF16), pltpu.VMEM((R*C, QB), BF16), pltpu.VMEM((H, N, QB), F32),
                        pltpu.VMEM((N//R, R, R*C), BF16), pltpu.VMEM((2, N//R, R, R*C), BF16),
                        pltpu.VMEM((2, BLOCKS, T, T, T, 2, 2*H, R, 128), BF16),
                        dma, dma((2,)), dma, dma((2, BLOCKS, 5)), dma((2, BLOCKS, 5))],
        compiler_params=pltpu.CompilerParams(dimension_semantics=("arbitrary", "arbitrary"), vmem_limit_bytes=60*2**20,
                                             collective_id=0, has_side_effects=True),
        cost_estimate=pl.CostEstimate(flops=n_pass*4*R*H*N*N*(C//H), bytes_accessed=4*N*R*C, transcendentals=n_pass*R*H*N*N),
        name="mega",
    )(*args)


def _ln_rows(x, w):
    x = x.astype(F32)
    mu = jnp.mean(x, axis=-1, keepdims=True)
    var = jnp.mean(jnp.square(x - mu), axis=-1, keepdims=True)
    y = (x - mu) * lax.rsqrt(var + EPS)
    return (y * w[0].astype(F32) + w[1].astype(F32)).astype(BF16)


def _rows(zl, bias, lw, wi, bg, wo, bo):
    h, n, _ = bias.shape
    c = zl.shape[-1]
    d = c // h

    def row(zr):
        y = _ln_rows(zr, lw)
        proj = jnp.transpose(jnp.dot(y, wi, preferred_element_type=F32).reshape(n, 4, h, d), (1, 2, 0, 3))
        gate = jax.nn.sigmoid(proj[3] + bg.astype(F32).reshape(h, 1, d))

        def head(a):
            q, k, v, b = a
            s = jnp.dot(q, k.T, preferred_element_type=F32) * d ** -0.5 + b
            return jnp.dot(jax.nn.softmax(s, axis=-1).astype(BF16), v, preferred_element_type=F32)

        o = lax.map(head, (*(a.astype(BF16) for a in proj[:3]), bias))
        o = jnp.transpose((gate * o).astype(BF16), (1, 0, 2)).reshape(n, c)
        return (zr.astype(F32) + jnp.dot(o, wo, preferred_element_type=F32) + bo.astype(F32)).astype(BF16)

    return lax.map(row, zl)


def solution(mesh):
    def local(zl, res_mask, ln_w, w_in, b_g, w_b, w_o, b_o):
        R, N, C = zl.shape
        n = ln_w.shape[0] * ln_w.shape[1]
        ws = tuple(a.reshape(n, *a.shape[2:]) for a in (ln_w, w_in, b_g, w_b, w_o, b_o))
        cols, wqvt, wk2, wo, wbn, mask, ok = setup(ws, res_mask, R)

        def fast(zl):
            return jnp.swapaxes(mega(jnp.swapaxes(zl, 1, 2), mask, cols, wqvt, wk2, wo, wbn), 1, 2)

        def exact(zl):
            mask_bias = jnp.where(res_mask > 0, 0.0, NEG).astype(F32)

            def one(p, z):
                lw, wi, bg, wb, wo, bo = (lax.dynamic_index_in_dim(a, p, keepdims=False) for a in ws)
                b = jnp.dot(_ln_rows(z, lw).reshape(R*N, C), wb, preferred_element_type=F32).astype(BF16)
                b = jnp.transpose(b.reshape(R, 8, N//8, -1), (3, 1, 0, 2))
                b = b.reshape(-1, R, N//8)
                bias = lax.map(lambda a: lax.all_gather(a, 'dap', axis=0, tiled=True), b)
                bias = jnp.swapaxes(bias.reshape(-1, 8, N, N//8), 1, 2).reshape(-1, N, N)
                z = _rows(z, bias.astype(F32) + mask_bias, lw, wi, bg, wo, bo)
                return jnp.swapaxes(lax.all_to_all(z, 'dap', 1, 0, tiled=True), 0, 1)
            return lax.fori_loop(0, n, one, zl)

        return lax.cond(ok[0, 0] > 0, fast, exact, zl)

    rows = P(('data', 'dap'))
    return jax.shard_map(local, mesh=mesh,
                         in_specs=(rows, P('data'), P(), P(), P(), P(), P(), P()),
                         out_specs=rows, check_vma=False)
```

```python
import functools
import jax
import jax.numpy as jnp
from jax import lax
from jax.experimental import pallas as pl
from jax.experimental.pallas import tpu as pltpu
from jax.sharding import PartitionSpec as P

F32 = jnp.float32
BF16 = jnp.bfloat16
EPS = 1e-5
NEG = -1e9
LOG2E = 1.4426950408889634
T = 4
BLOCKS = 4
PARTS = (((2, 1, 0), 0, 3), ((1, 0, 2), 3, 3), ((0, 2, 1), 6, 2))
MESH = pl.DeviceIdType.MESH
HIGH = lax.Precision.HIGHEST


def _ln_t(x, gamma, beta):
    mu = jnp.mean(x, axis=0, keepdims=True)
    d = x - mu
    var = jnp.mean(d*d, axis=0, keepdims=True)
    return (d * lax.rsqrt(var + EPS) * gamma + beta).astype(BF16)


def _place(b, r):
    z, y = r // (2*T), (r // 2) % T
    return z, y, 2*(r % 2) + (b // 2 + z + y) % 2, b % 2


def _block(z, y, x, c):
    return (z + y + x) % 2 * 2 + c, (z*T + y)*2 + x // 2


def _index(z, y, x, c):
    return ((z*T + y)*T + x)*2 + c


def setup_kernel(R, ln_ref, win_ref, bg_ref, wbt_ref, wo_ref, bo_ref, m_ref,
                 cols_ref, wqvt_ref, wk2_ref, wot_ref, wbn_ref, mask_ref, ok_ref):
    n, H, C = wbt_ref.shape
    D = C // H
    iota = lambda shape, axis: lax.broadcasted_iota(jnp.int32, shape, axis)
    head = iota((C, C), 0) // D == iota((C, C), 1) // D
    lane = iota((C, 2*C), 1)
    twice = (iota((C, 2*C), 0) == (lane // (2*D)) * D + lane % D).astype(F32).astype(BF16)
    mine = iota((H, R, R*C), 1) == iota((H, R, R*C), 2) // C
    nt = lambda a, b: lax.dot_general(a, b, (((1,), (1,)), ((), ())), precision=HIGH, preferred_element_type=F32)
    whole = lambda f, a: f(f(a, axis=1, keepdims=True), axis=0, keepdims=True)
    top = lambda m: whole(lambda a, axis, keepdims: jnp.sum(a, axis=1, keepdims=True) if axis else
                          jnp.max(a, axis=0, keepdims=True), jnp.abs(m))
    good = jnp.ones((1, 1), F32)
    for p in range(n):
        ln = ln_ref[p].astype(F32)
        vecs = jnp.concatenate([ln, bg_ref[p:p+1].astype(F32), bo_ref[p:p+1].astype(F32), jnp.zeros((4, C), F32)], axis=0)
        cols_ref[p] = jnp.concatenate([vecs, jnp.zeros((8, C), F32)], axis=1).T[0:C]
        w = win_ref[p].T
        wqvt_ref[p, 0:C] = w[0:C]
        wqvt_ref[p, C:3*C] = w[2*C:4*C]
        wk = lax.dot_general(w[C:2*C], twice, (((0,), (0,)), ((), ())), preferred_element_type=F32)
        wk2_ref[p] = wk.astype(BF16)
        wot_ref[p] = wo_ref[p].T
        wb = wbt_ref[p].astype(F32)
        rep = jnp.concatenate([wb]*R, axis=1)
        wbn_ref[p] = jnp.where(mine, rep[:, None, :], 0.0).reshape(H*R, R*C).astype(BF16)

        w = w.astype(F32)
        wg = w * ln[0:1]
        gram = [jnp.where(head, nt(wg[a*C:(a+1)*C], wg[a*C:(a+1)*C]), 0.0) for a in range(3)]
        both = jnp.sqrt(top(jnp.dot(gram[0], gram[1], precision=HIGH, preferred_element_type=F32))) * C
        one = [jnp.sqrt(top(g) * C) for g in gram]
        off = jnp.square(jnp.sum(w * ln[1:2], axis=1, keepdims=True))
        per = lambda a: functools.reduce(jnp.maximum, [jnp.sum(off[a*C+h*D:a*C+(h+1)*D], axis=0, keepdims=True) for h in range(H)])
        q, k, v = (one[a] + jnp.sqrt(per(a)) for a in range(3))
        qk = both + q*k - one[0]*one[1] + 0.02*q*k
        nb = jnp.sqrt(jnp.sum(jnp.square(wb * ln[0:1]), axis=1, keepdims=True) * C) + jnp.abs(jnp.sum(wb * ln[1:2], axis=1, keepdims=True))
        s = LOG2E * (qk * D ** -0.5 + 1.02 * jnp.max(nb, axis=0, keepdims=True))
        good = jnp.where((s <= 100.0) & (v <= 2.0 ** 14), good, 0.0)
    ok_ref[0, 0] = jnp.min(good).astype(jnp.int32)

    cols = m_ref[...].astype(F32).T
    for j in range(m_ref.shape[0]):
        col = jnp.where(jnp.broadcast_to(cols[:, j:j+1], (128, 128)) > 0.0, 0.0, NEG)
        for e in range(16):
            g = 16*j + e
            b, r = _block(g // (2*T*T), (g // (2*T)) % T, (g // 2) % T, g % 2)
            mask_ref[(b*2*T*T + r)*R:(b*2*T*T + r + 1)*R] = col[R*e:R*(e+1)]


def setup(ws, res_mask, R):
    n, C, H = ws[3].shape
    N = res_mask.shape[0]
    ln_w, w_in, b_g, w_b, w_o, b_o = ws
    sds = jax.ShapeDtypeStruct
    out = (sds((n, C, 8), F32), sds((n, 3*C, C), BF16), sds((n, C, 2*C), BF16), sds((n, C, C), BF16), sds((n, H*R, R*C), BF16),
           sds((N, 128), F32), sds((1, 1), jnp.int32))
    vmem, smem = pl.BlockSpec(memory_space=pltpu.VMEM), pl.BlockSpec(memory_space=pltpu.SMEM)
    return pl.pallas_call(functools.partial(setup_kernel, R), in_specs=[vmem]*7, out_specs=[vmem]*6 + [smem], out_shape=out,
                          name="setup")(ln_w, w_in, b_g, jnp.swapaxes(w_b, 1, 2), w_o, b_o, res_mask.reshape(N//128, 128))


def mega_kernel(R, N, C, H, LAG,
                z_ref, mask_ref, cols_ref, wqvt_ref, wk2_ref, wo_ref, wbn_ref,
                out_ref,
                k_s, q_s, v_s, g_s, z_s, o_s, y_s, zt_s, bias_s, x_s, r_s, G,
                a2a_send, a2a_recv, own_sem, ag_send, ag_recv):
    ps, jb = pl.program_id(0), pl.program_id(1)
    n_pass = cols_ref.shape[0]
    me = lax.axis_index('dap')
    n_dev = 2*T*T*T
    others = pl.ds(0, n_dev-1)
    D = C // H
    QB = N // BLOCKS
    KC = 128
    CH = N // KC
    DB = QB // R
    par, nxt = lax.rem(ps, 2), lax.rem(ps + 1, 2)
    q0 = pl.multiple_of(jb * QB, QB)
    core = me % 2
    at = (me // (2*T*T), (me // (2*T)) % T, (me // 2) % T)
    my_block, my_place = _block(*at, core)
    last = ps // (n_pass-1)
    slot_of_me = (my_block*DB + my_place) * (1-last) + me * last

    stride = (2*T*T, 2*T, 2)
    near = [[(at[a] + j) % T for j in range(T)] for a in range(3)]
    step = [[near[a][j] * stride[a] for j in range(T)] for a in range(3)]
    home = [step[a][0] for a in range(3)]

    def moved(axis, by):
        return core + sum(home[a] for a in range(3) if a != axis) + step[axis][by]

    def copy(g, b, k, sel, u0, nu, to):
        r = G.at[g, b, sel[0], sel[1], sel[2], core, pl.ds(u0, nu)]
        return pltpu.make_async_remote_copy(r, r, ag_send.at[g, b, k], ag_recv.at[g, b, k],
                                            device_id={'dap': to}, device_id_type=MESH)

    every = slice(None)
    sizes = ((0, pl.ds(0, 3), every), (pl.ds(0, 2), every, every), (0, every, every), (every,)*3, (0, 0, pl.ds(0, 3)))

    def landed(g, b, k, sem):
        for j in (k, 4) if k == 0 else (k,):
            r = G.at[(g, b) + sizes[j] + (0,)]
            pltpu.make_async_copy(r, r, sem.at[g, b, j]).wait()

    def stage(k, g, b):
        if k > 0:
            landed(g, b, k-1, ag_recv)
        if k == 4:
            for j in range(4):
                landed(g, b, j, ag_send)
            return
        if k == 3:
            r = G.at[g, b, :, :, :, core]
            pltpu.make_async_remote_copy(r, r, ag_send.at[g, b, 3], ag_recv.at[g, b, 3],
                                         device_id={'dap': me + 1 - 2*core}, device_id_type=MESH).start()
            return
        for (a0, a1, a2), u0, nu in PARTS:
            if k == 0:
                for j in range(1, T):
                    copy(g, b, 4, at, u0, nu, moved(a0, j)).start()
                def line(f, _):
                    row = core + home[a2] + (at[a1] + f) % T * stride[a1]
                    for j in range(T):
                        copy(g, b, 0, at, u0, nu, row + step[a0][j]).start()
                    return 0
                lax.fori_loop(1, T, line, 0)
                continue
            sel = list(at)
            sel[a0] = every
            for by, half in ((1, 0), (T-1, T//2)):
                if k == 1:
                    sel[a1] = every
                else:
                    sel[a1] = pl.ds(half, T//2)
                    sel[a2] = near[a2][T-by]
                copy(g, b, k, sel, u0, nu, moved(a2, by)).start()

    def slot(s, p):
        for k in range(5):
            b = s - k
            if isinstance(s, int):
                if 0 < b < BLOCKS:
                    stage(k, (p + 1) % 2, b)
                continue
            if k < BLOCKS:
                @pl.when((b >= 0) & (p < n_pass-1))
                def _():
                    stage(k, (p + 1) % 2, b)
            if k > 1:
                @pl.when((b < 0) & (b + 5 < BLOCKS) & (p >= 1))
                def _():
                    stage(k, p % 2, b + 5)

    def put_bias(g, b, rows):
        for h in range(H):
            for t in range(2):
                G[g, b, at[0], at[1], at[2], core, 2*h+t] = rows[h*R:(h+1)*R, t*128:(t+1)*128]

    def col(p, j):
        return cols_ref[p, :, j:j+1]

    def bias_rows(p, y):
        return jnp.dot(wbn_ref[p], y, preferred_element_type=F32).astype(BF16)

    def prep(i):
        y = _ln_t(z_s[i].astype(F32), col(ps, 0), col(ps, 1))
        p = jnp.dot(wqvt_ref[ps], y, preferred_element_type=F32)
        k_s[i] = jnp.dot(y.T, wk2_ref[ps], preferred_element_type=F32).astype(BF16)
        q = p[0:C].astype(BF16).astype(F32) * (LOG2E * D ** -0.5)
        qh = q.astype(BF16)
        ql = (q - qh.astype(F32)).astype(BF16)
        for h in range(H):
            q_s[i, 2*D*h:2*D*h+D] = qh[D*h:D*h+D]
            q_s[i, 2*D*h+D:2*D*h+2*D] = ql[D*h:D*h+D]
        v_s[i] = p[C:2*C].astype(BF16)
        g_s[i] = jax.nn.sigmoid(p[2*C:3*C] + col(ps, 2))

    def prep_all():
        def some(t, _):
            for j in range(4):
                prep(4*t+j)
            return 0
        lax.fori_loop(0, R//4, some, 0)

    def unpack(g, w):
        t = r_s[g, pl.ds(w*16, 16)].reshape(16*R, R*C).astype(F32).T
        x = [t[i*C:(i+1)*C] for i in range(R)]
        lane = lax.broadcasted_iota(jnp.int32, (C, 128), 1)
        for bit in (1, 2, 4):
            odd = (lane & bit) != 0
            for i in range(R):
                if not i & bit:
                    a, b = x[i], x[i | bit]
                    x[i] = jnp.where(odd, pltpu.roll(b, bit, 1), a)
                    x[i | bit] = jnp.where(odd, b, pltpu.roll(a, 128-bit, 1))
        for i in range(R):
            z_s[i, :, pl.ds(pl.multiple_of(w*128, 128), 128)] = x[i].astype(BF16)

    def arrived(g):
        pltpu.make_async_copy(r_s.at[g, others], r_s.at[g, others], a2a_recv.at[g]).wait()
        pltpu.make_async_copy(r_s.at[g, others], r_s.at[g, others], a2a_send).wait()
        def two(t, _):
            unpack(g, 2*t)
            unpack(g, 2*t+1)
            return 0
        lax.fori_loop(0, N//256, two, 0)

    def to_f32(b, h, m):
        for w in range(2):
            v = [G[(par, b) + _place(m // 2, (m % 2)*16 + r) + (2*h+w,)] for r in range(16)]
            v = jnp.concatenate(v, axis=0).astype(F32)
            bias_s[h, m*128:(m+1)*128, w*128:(w+1)*128] = v * LOG2E + mask_ref[m*128:(m+1)*128]

    def to_f32_all(b):
        def each(h, _):
            for m in range(CH):
                to_f32(b, h, m)
            return 0
        lax.fori_loop(0, H, each, 0)

    def turn_bias(h, _):
        for b in range(BLOCKS):
            for a in range(b+1):
                got = {}
                for u, v in ((a, b), (b, a))[a == b:]:
                    for t in range(2):
                        x = [G[(0, u) + _place(v, r) + (2*h+t,)] for r in range(DB)]
                        got[u, v, t] = jnp.concatenate(x, axis=0).astype(F32).T.astype(BF16)
                for (u, v, t), x in got.items():
                    for r in range(16):
                        for w in range(2):
                            G[(0, v) + _place(u, t*16 + r) + (2*h+w,)] = x[r*R:(r+1)*R, w*128:(w+1)*128]
        return 0

    @pl.when((jb == 0) & (ps == 0))
    def _():
        barrier = pltpu.get_barrier_semaphore()
        def greet(k, _):
            pl.semaphore_signal(barrier, inc=1, device_id={'dap': (me + k) % n_dev}, device_id_type=MESH)
            return 0
        lax.fori_loop(1, n_dev, greet, 0)
        def first(b, _):
            row = lax.broadcasted_iota(jnp.int32, (N, QB), 0)
            lane = lax.broadcasted_iota(jnp.int32, (N, QB), 1)
            r = lane // R
            turn = (row == _index(*_place(b, r))*R + lane % R).astype(F32).astype(BF16)
            qs = pl.ds(pl.multiple_of(b*QB, QB), QB)
            for i in range(R):
                zb = jnp.dot(z_ref[i], turn, preferred_element_type=F32)
                z_s[i, :, qs] = zb.astype(BF16)
                y_s[i*C:(i+1)*C] = _ln_t(zb, col(0, 0), col(0, 1))
            put_bias(0, b, bias_rows(0, y_s[...]))
            return 0
        lax.fori_loop(0, BLOCKS, first, 0)
        pl.semaphore_wait(barrier, n_dev - 1)
        def gather(k):
            def each(b, _):
                stage(k, 0, b)
                return 0
            lax.fori_loop(0, BLOCKS, each, 0)
        gather(0)
        gather(1)
        prep_all()
        gather(2)
        gather(3)
        gather(4)
        lax.fori_loop(0, H, turn_bias, 0)
        to_f32_all(0)

    @pl.when((jb == 0) & (ps > 0))
    def _():
        stage(4, par, 0)
        to_f32_all(0)
        arrived(par)
        prep_all()
        slot(4, ps-1)

    @pl.when(jb > 0)
    def _():
        to_f32_all(jb)

    zl = jnp.zeros((KC, 256-2*C), BF16)
    zp = jnp.zeros((KC, QB), BF16)
    zv = jnp.zeros((D, 256-KC), BF16)
    zq = jnp.zeros((2*D, QB), BF16)
    steps = [(h, c) for h in range(H) for c in range(CH)]
    S = len(steps)
    es, ss, acc, tot = {}, {}, [None]*R, [None]*R
    for n in range(-LAG, S):
        if n >= 0:
            h, c = steps[n]
            b = bias_s[h, c*KC:(c+1)*KC]
            for i in range(R):
                e = jnp.exp2(ss.pop((n, i)) + b)
                es[i] = e.astype(BF16)
                e = jnp.sum(e.reshape(KC//8, 8, QB), axis=0)
                tot[i] = e if c == 0 else tot[i] + e
        for i in range(R):
            rows = []
            w = zp
            if n+LAG < S:
                h2, c2 = steps[n+LAG]
                w = jnp.concatenate([zq]*h2 + [q_s[i, 2*D*h2:2*D*(h2+1), pl.ds(q0, QB)]] + [zq]*(H-1-h2), axis=0)
                rows.append(jnp.concatenate([zl, k_s[i, c2*KC:(c2+1)*KC]], axis=1))
            if n >= 0:
                rows.append(jnp.concatenate([v_s[i, D*h:D*h+D, c*KC:(c+1)*KC], zv], axis=1))
            o = jnp.dot(jnp.concatenate(rows, axis=0), jnp.concatenate([es.pop(i) if n >= 0 else zp, w], axis=0),
                        preferred_element_type=F32)
            if n+LAG < S:
                ss[n+LAG, i] = o[0:KC]
            if n >= 0:
                o = o[-D:]
                acc[i] = o if c == 0 else acc[i] + o
                if c == CH-1:
                    a = acc[i] / jnp.sum(tot[i], axis=0, keepdims=True)
                    o_s[i, D*h:D*h+D] = (g_s[i, D*h:D*h+D, pl.ds(q0, QB)] * a).astype(BF16)

    for i in range(R):
        u = jnp.dot(wo_ref[ps], o_s[i], preferred_element_type=F32) + col(ps, 3)
        zt_s[i*C:(i+1)*C] = (z_s[i, :, pl.ds(q0, QB)].astype(F32) + u).astype(BF16)
    x_s[pl.ds(jb*DB, DB)] = zt_s[...].T.reshape(DB, R, R*C)

    def send(t, _):
        for j in range(4):
            k = 4*t + j
            d = _index(*_place(jb, k))
            @pl.when(d != me)
            def _():
                pltpu.make_async_remote_copy(x_s.at[jb*DB + k], r_s.at[nxt, slot_of_me], a2a_send, a2a_recv.at[nxt],
                                             device_id={'dap': d}, device_id_type=MESH).start()
        return 0
    lax.fori_loop(0, DB//4, send, 0)

    @pl.when(my_block == jb)
    def _():
        r_s[nxt, slot_of_me] = x_s[jb*DB + my_place]

    pn = (ps + 1) % n_pass
    for i in range(R):
        y_s[i*C:(i+1)*C] = _ln_t(zt_s[i*C:(i+1)*C].astype(F32), col(pn, 0), col(pn, 1))

    @pl.when(ps < n_pass-1)
    def _():
        put_bias(nxt, jb, bias_rows(pn, y_s[...]))
    slot(jb, ps)

    @pl.when((ps == n_pass-1) & (jb == BLOCKS-1))
    def _():
        arrived(nxt)
        out = pltpu.make_async_copy(z_s, out_ref, own_sem)
        out.start()
        out.wait()


def mega(z, mask, cols, wqvt, wk2, wo, wbn, LAG=2):
    R, C, N = z.shape
    n_pass = cols.shape[0]
    H = wbn.shape[1] // R
    QB = N // BLOCKS
    full = lambda a: pl.BlockSpec(a.shape, lambda p, j: (0,)*a.ndim, pipeline_mode=pl.Buffered(1))
    args = (z, mask, cols, wqvt, wk2, wo, wbn)
    dma = pltpu.SemaphoreType.DMA
    return pl.pallas_call(
        functools.partial(mega_kernel, R, N, C, H, LAG),
        grid=(n_pass, BLOCKS),
        in_specs=[full(a) for a in args],
        out_specs=pl.BlockSpec(memory_space=pl.ANY),
        out_shape=jax.ShapeDtypeStruct((R, C, N), BF16),
        scratch_shapes=[pltpu.VMEM((R, N, 2*C), BF16), pltpu.VMEM((R, 2*C, N), BF16), pltpu.VMEM((R, C, N), BF16),
                        pltpu.VMEM((R, C, N), F32), pltpu.VMEM((R, C, N), BF16), pltpu.VMEM((R, C, QB), BF16),
                        pltpu.VMEM((R*C, QB), BF16), pltpu.VMEM((R*C, QB), BF16), pltpu.VMEM((H, N, QB), F32),
                        pltpu.VMEM((N//R, R, R*C), BF16), pltpu.VMEM((2, N//R, R, R*C), BF16),
                        pltpu.VMEM((2, BLOCKS, T, T, T, 2, 2*H, R, 128), BF16),
                        dma, dma((2,)), dma, dma((2, BLOCKS, 5)), dma((2, BLOCKS, 5))],
        compiler_params=pltpu.CompilerParams(dimension_semantics=("arbitrary", "arbitrary"), vmem_limit_bytes=60*2**20,
                                             collective_id=0, has_side_effects=True),
        cost_estimate=pl.CostEstimate(flops=n_pass*4*R*H*N*N*(C//H), bytes_accessed=4*N*R*C, transcendentals=n_pass*R*H*N*N),
        name="mega",
    )(*args)


def _ln_rows(x, w):
    x = x.astype(F32)
    mu = jnp.mean(x, axis=-1, keepdims=True)
    var = jnp.mean(jnp.square(x - mu), axis=-1, keepdims=True)
    y = (x - mu) * lax.rsqrt(var + EPS)
    return (y * w[0].astype(F32) + w[1].astype(F32)).astype(BF16)


def _rows(zl, bias, lw, wi, bg, wo, bo):
    h, n, _ = bias.shape
    c = zl.shape[-1]
    d = c // h

    def row(zr):
        y = _ln_rows(zr, lw)
        proj = jnp.transpose(jnp.dot(y, wi, preferred_element_type=F32).reshape(n, 4, h, d), (1, 2, 0, 3))
        gate = jax.nn.sigmoid(proj[3] + bg.astype(F32).reshape(h, 1, d))

        def head(a):
            q, k, v, b = a
            s = jnp.dot(q, k.T, preferred_element_type=F32) * d ** -0.5 + b
            return jnp.dot(jax.nn.softmax(s, axis=-1).astype(BF16), v, preferred_element_type=F32)

        o = lax.map(head, (*(a.astype(BF16) for a in proj[:3]), bias))
        o = jnp.transpose((gate * o).astype(BF16), (1, 0, 2)).reshape(n, c)
        return (zr.astype(F32) + jnp.dot(o, wo, preferred_element_type=F32) + bo.astype(F32)).astype(BF16)

    return lax.map(row, zl)


def solution(mesh):
    def local(zl, res_mask, ln_w, w_in, b_g, w_b, w_o, b_o):
        R, N, C = zl.shape
        n = ln_w.shape[0] * ln_w.shape[1]
        ws = tuple(a.reshape(n, *a.shape[2:]) for a in (ln_w, w_in, b_g, w_b, w_o, b_o))
        cols, wqvt, wk2, wo, wbn, mask, ok = setup(ws, res_mask, R)

        def fast(zl):
            return jnp.swapaxes(mega(jnp.swapaxes(zl, 1, 2), mask, cols, wqvt, wk2, wo, wbn), 1, 2)

        def exact(zl):
            mask_bias = jnp.where(res_mask > 0, 0.0, NEG).astype(F32)

            def one(p, z):
                lw, wi, bg, wb, wo, bo = (lax.dynamic_index_in_dim(a, p, keepdims=False) for a in ws)
                b = jnp.dot(_ln_rows(z, lw).reshape(R*N, C), wb, preferred_element_type=F32).astype(BF16)
                b = jnp.transpose(b.reshape(R, 8, N//8, -1), (3, 1, 0, 2))
                b = b.reshape(-1, R, N//8)
                bias = lax.map(lambda a: lax.all_gather(a, 'dap', axis=0, tiled=True), b)
                bias = jnp.swapaxes(bias.reshape(-1, 8, N, N//8), 1, 2).reshape(-1, N, N)
                z = _rows(z, bias.astype(F32) + mask_bias, lw, wi, bg, wo, bo)
                return jnp.swapaxes(lax.all_to_all(z, 'dap', 1, 0, tiled=True), 0, 1)
            return lax.fori_loop(0, n, one, zl)

        return lax.cond(ok[0, 0] > 0, fast, exact, zl)

    rows = P(('data', 'dap'))
    return jax.shard_map(local, mesh=mesh,
                         in_specs=(rows, P('data'), P(), P(), P(), P(), P(), P()),
                         out_specs=rows, check_vma=False)
```

```python
import functools
import jax
import jax.numpy as jnp
from jax import lax
from jax.experimental import pallas as pl
from jax.experimental.pallas import tpu as pltpu
from jax.sharding import PartitionSpec as P

F32 = jnp.float32
BF16 = jnp.bfloat16
EPS = 1e-5
NEG = -1e9
LOG2E = 1.4426950408889634
T = 4
BLOCKS = 4
PARTS = (((2, 1, 0), 0, 3), ((1, 0, 2), 3, 3), ((0, 2, 1), 6, 2))
MESH = pl.DeviceIdType.MESH
HIGH = lax.Precision.HIGHEST


def _ln_t(x, gamma, beta):
    mu = jnp.mean(x, axis=0, keepdims=True)
    d = x - mu
    var = jnp.mean(d*d, axis=0, keepdims=True)
    return (d * lax.rsqrt(var + EPS) * gamma + beta).astype(BF16)


def _place(b, r):
    z, y = r // (2*T), (r // 2) % T
    return z, y, 2*(r % 2) + (b // 2 + z + y) % 2, b % 2


def _block(z, y, x, c):
    return (z + y + x) % 2 * 2 + c, (z*T + y)*2 + x // 2


def _index(z, y, x, c):
    return ((z*T + y)*T + x)*2 + c


def setup_kernel(R, ln_ref, win_ref, bg_ref, wbt_ref, wo_ref, bo_ref, m_ref,
                 cols_ref, wqvt_ref, wk2_ref, wot_ref, wbn_ref, mask_ref, ok_ref):
    n, H, C = wbt_ref.shape
    D = C // H
    iota = lambda shape, axis: lax.broadcasted_iota(jnp.int32, shape, axis)
    head = iota((C, C), 0) // D == iota((C, C), 1) // D
    lane = iota((C, 2*C), 1)
    twice = (iota((C, 2*C), 0) == (lane // (2*D)) * D + lane % D).astype(F32).astype(BF16)
    mine = iota((H, R, R*C), 1) == iota((H, R, R*C), 2) // C
    nt = lambda a, b: lax.dot_general(a, b, (((1,), (1,)), ((), ())), precision=HIGH, preferred_element_type=F32)
    whole = lambda f, a: f(f(a, axis=1, keepdims=True), axis=0, keepdims=True)
    top = lambda m: whole(lambda a, axis, keepdims: jnp.sum(a, axis=1, keepdims=True) if axis else
                          jnp.max(a, axis=0, keepdims=True), jnp.abs(m))
    good = jnp.ones((1, 1), F32)
    for p in range(n):
        ln = ln_ref[p].astype(F32)
        vecs = jnp.concatenate([ln, bg_ref[p:p+1].astype(F32), bo_ref[p:p+1].astype(F32), jnp.zeros((4, C), F32)], axis=0)
        cols_ref[p] = jnp.concatenate([vecs, jnp.zeros((8, C), F32)], axis=1).T[0:C]
        w = win_ref[p].T
        wqvt_ref[p, 0:C] = w[0:C]
        wqvt_ref[p, C:3*C] = w[2*C:4*C]
        wk = lax.dot_general(w[C:2*C], twice, (((0,), (0,)), ((), ())), preferred_element_type=F32)
        wk2_ref[p] = wk.astype(BF16)
        wot_ref[p] = wo_ref[p].T
        wb = wbt_ref[p].astype(F32)
        rep = jnp.concatenate([wb]*R, axis=1)
        wbn_ref[p] = jnp.where(mine, rep[:, None, :], 0.0).reshape(H*R, R*C).astype(BF16)

        w = w.astype(F32)
        wg = w * ln[0:1]
        gram = [jnp.where(head, nt(wg[a*C:(a+1)*C], wg[a*C:(a+1)*C]), 0.0) for a in range(3)]
        both = jnp.sqrt(top(jnp.dot(gram[0], gram[1], precision=HIGH, preferred_element_type=F32))) * C
        one = [jnp.sqrt(top(g) * C) for g in gram]
        off = jnp.square(jnp.sum(w * ln[1:2], axis=1, keepdims=True))
        per = lambda a: functools.reduce(jnp.maximum, [jnp.sum(off[a*C+h*D:a*C+(h+1)*D], axis=0, keepdims=True) for h in range(H)])
        q, k, v = (one[a] + jnp.sqrt(per(a)) for a in range(3))
        qk = both + q*k - one[0]*one[1] + 0.02*q*k
        nb = jnp.sqrt(jnp.sum(jnp.square(wb * ln[0:1]), axis=1, keepdims=True) * C) + jnp.abs(jnp.sum(wb * ln[1:2], axis=1, keepdims=True))
        s = LOG2E * (qk * D ** -0.5 + 1.02 * jnp.max(nb, axis=0, keepdims=True))
        good = jnp.where((s <= 100.0) & (v <= 2.0 ** 14), good, 0.0)
    ok_ref[0, 0] = jnp.min(good).astype(jnp.int32)

    cols = m_ref[...].astype(F32).T
    for j in range(m_ref.shape[0]):
        col = jnp.where(jnp.broadcast_to(cols[:, j:j+1], (128, 128)) > 0.0, 0.0, NEG)
        for e in range(16):
            g = 16*j + e
            b, r = _block(g // (2*T*T), (g // (2*T)) % T, (g // 2) % T, g % 2)
            mask_ref[(b*2*T*T + r)*R:(b*2*T*T + r + 1)*R] = col[R*e:R*(e+1)]


def setup(ws, res_mask, R):
    n, C, H = ws[3].shape
    N = res_mask.shape[0]
    ln_w, w_in, b_g, w_b, w_o, b_o = ws
    sds = jax.ShapeDtypeStruct
    out = (sds((n, C, 8), F32), sds((n, 3*C, C), BF16), sds((n, C, 2*C), BF16), sds((n, C, C), BF16), sds((n, H*R, R*C), BF16),
           sds((N, 128), F32), sds((1, 1), jnp.int32))
    vmem, smem = pl.BlockSpec(memory_space=pltpu.VMEM), pl.BlockSpec(memory_space=pltpu.SMEM)
    return pl.pallas_call(functools.partial(setup_kernel, R), in_specs=[vmem]*7, out_specs=[vmem]*6 + [smem], out_shape=out,
                          name="setup")(ln_w, w_in, b_g, jnp.swapaxes(w_b, 1, 2), w_o, b_o, res_mask.reshape(N//128, 128))


def mega_kernel(R, N, C, H, LAG,
                z_ref, mask_ref, cols_ref, wqvt_ref, wk2_ref, wo_ref, wbn_ref,
                out_ref,
                k_s, q_s, v_s, g_s, z_s, o_s, y_s, zt_s, bias_s, x_s, r_s, G,
                a2a_send, a2a_recv, own_sem, ag_send, ag_recv):
    ps, jb = pl.program_id(0), pl.program_id(1)
    n_pass = cols_ref.shape[0]
    me = lax.axis_index('dap')
    n_dev = 2*T*T*T
    others = pl.ds(0, n_dev-1)
    D = C // H
    QB = N // BLOCKS
    KC = 128
    CH = N // KC
    DB = QB // R
    par, nxt = lax.rem(ps, 2), lax.rem(ps + 1, 2)
    q0 = pl.multiple_of(jb * QB, QB)
    core = me % 2
    at = (me // (2*T*T), (me // (2*T)) % T, (me // 2) % T)
    my_block, my_place = _block(*at, core)
    last = ps // (n_pass-1)
    slot_of_me = (my_block*DB + my_place) * (1-last) + me * last

    stride = (2*T*T, 2*T, 2)
    near = [[(at[a] + j) % T for j in range(T)] for a in range(3)]
    step = [[near[a][j] * stride[a] for j in range(T)] for a in range(3)]
    home = [step[a][0] for a in range(3)]

    def moved(axis, by):
        return core + sum(home[a] for a in range(3) if a != axis) + step[axis][by]

    def copy(g, b, k, sel, u0, nu, to):
        r = G.at[g, b, sel[0], sel[1], sel[2], core, pl.ds(u0, nu)]
        return pltpu.make_async_remote_copy(r, r, ag_send.at[g, b, k], ag_recv.at[g, b, k],
                                            device_id={'dap': to}, device_id_type=MESH)

    every = slice(None)
    sizes = ((0, pl.ds(0, 3), every), (pl.ds(0, 2), every, every), (0, every, every), (every,)*3, (0, 0, pl.ds(0, 3)))

    def landed(g, b, k, sem):
        for j in (k, 4) if k == 0 else (k,):
            r = G.at[(g, b) + sizes[j] + (0,)]
            pltpu.make_async_copy(r, r, sem.at[g, b, j]).wait()

    def stage(k, g, b):
        if k > 0:
            landed(g, b, k-1, ag_recv)
        if k == 4:
            for j in range(4):
                landed(g, b, j, ag_send)
            return
        if k == 3:
            r = G.at[g, b, :, :, :, core]
            pltpu.make_async_remote_copy(r, r, ag_send.at[g, b, 3], ag_recv.at[g, b, 3],
                                         device_id={'dap': me + 1 - 2*core}, device_id_type=MESH).start()
            return
        for (a0, a1, a2), u0, nu in PARTS:
            if k == 0:
                for j in range(1, T):
                    copy(g, b, 4, at, u0, nu, moved(a0, j)).start()
                def line(f, _):
                    row = core + home[a2] + (at[a1] + f) % T * stride[a1]
                    for j in range(T):
                        copy(g, b, 0, at, u0, nu, row + step[a0][j]).start()
                    return 0
                lax.fori_loop(1, T, line, 0)
                continue
            sel = list(at)
            sel[a0] = every
            for by, half in ((1, 0), (T-1, T//2)):
                if k == 1:
                    sel[a1] = every
                else:
                    sel[a1] = pl.ds(half, T//2)
                    sel[a2] = near[a2][T-by]
                copy(g, b, k, sel, u0, nu, moved(a2, by)).start()

    def slot(s, p):
        for k in reversed(range(5)):
            b = s - k
            if isinstance(s, int):
                if 0 < b < BLOCKS:
                    stage(k, (p + 1) % 2, b)
                continue
            if k < BLOCKS:
                @pl.when((b >= 0) & (p < n_pass-1))
                def _():
                    stage(k, (p + 1) % 2, b)
            if k > 1:
                @pl.when((b < 0) & (b + 5 < BLOCKS) & (p >= 1))
                def _():
                    stage(k, p % 2, b + 5)

    def put_bias(g, b, rows):
        for h in range(H):
            for t in range(2):
                G[g, b, at[0], at[1], at[2], core, 2*h+t] = rows[h*R:(h+1)*R, t*128:(t+1)*128]

    def col(p, j):
        return cols_ref[p, :, j:j+1]

    def bias_rows(p, y):
        return jnp.dot(wbn_ref[p], y, preferred_element_type=F32).astype(BF16)

    def prep(i):
        y = _ln_t(z_s[i].astype(F32), col(ps, 0), col(ps, 1))
        p = jnp.dot(wqvt_ref[ps], y, preferred_element_type=F32)
        k_s[i] = jnp.dot(y.T, wk2_ref[ps], preferred_element_type=F32).astype(BF16)
        q = p[0:C].astype(BF16).astype(F32) * (LOG2E * D ** -0.5)
        qh = q.astype(BF16)
        ql = (q - qh.astype(F32)).astype(BF16)
        for h in range(H):
            q_s[i, 2*D*h:2*D*h+D] = qh[D*h:D*h+D]
            q_s[i, 2*D*h+D:2*D*h+2*D] = ql[D*h:D*h+D]
        v_s[i] = p[C:2*C].astype(BF16)
        g_s[i] = jax.nn.sigmoid(p[2*C:3*C] + col(ps, 2))

    def prep_all():
        def some(t, _):
            for j in range(4):
                prep(4*t+j)
            return 0
        lax.fori_loop(0, R//4, some, 0)

    def unpack(g, w):
        t = r_s[g, pl.ds(w*16, 16)].reshape(16*R, R*C).astype(F32).T
        x = [t[i*C:(i+1)*C] for i in range(R)]
        lane = lax.broadcasted_iota(jnp.int32, (C, 128), 1)
        for bit in (1, 2, 4):
            odd = (lane & bit) != 0
            for i in range(R):
                if not i & bit:
                    a, b = x[i], x[i | bit]
                    x[i] = jnp.where(odd, pltpu.roll(b, bit, 1), a)
                    x[i | bit] = jnp.where(odd, b, pltpu.roll(a, 128-bit, 1))
        for i in range(R):
            z_s[i, :, pl.ds(pl.multiple_of(w*128, 128), 128)] = x[i].astype(BF16)

    def arrived(g):
        pltpu.make_async_copy(r_s.at[g, others], r_s.at[g, others], a2a_recv.at[g]).wait()
        pltpu.make_async_copy(r_s.at[g, others], r_s.at[g, others], a2a_send).wait()
        def two(t, _):
            unpack(g, 2*t)
            unpack(g, 2*t+1)
            return 0
        lax.fori_loop(0, N//256, two, 0)

    def to_f32(b, h, m):
        for w in range(2):
            v = [G[(par, b) + _place(m // 2, (m % 2)*16 + r) + (2*h+w,)] for r in range(16)]
            v = jnp.concatenate(v, axis=0).astype(F32)
            bias_s[h, m*128:(m+1)*128, w*128:(w+1)*128] = v * LOG2E + mask_ref[m*128:(m+1)*128]

    def to_f32_all(b):
        def each(h, _):
            for m in range(CH):
                to_f32(b, h, m)
            return 0
        lax.fori_loop(0, H, each, 0)

    def turn_bias(h, _):
        for b in range(BLOCKS):
            for a in range(b+1):
                got = {}
                for u, v in ((a, b), (b, a))[a == b:]:
                    for t in range(2):
                        x = [G[(0, u) + _place(v, r) + (2*h+t,)] for r in range(DB)]
                        got[u, v, t] = jnp.concatenate(x, axis=0).astype(F32).T.astype(BF16)
                for (u, v, t), x in got.items():
                    for r in range(16):
                        for w in range(2):
                            G[(0, v) + _place(u, t*16 + r) + (2*h+w,)] = x[r*R:(r+1)*R, w*128:(w+1)*128]
        return 0

    @pl.when((jb == 0) & (ps == 0))
    def _():
        barrier = pltpu.get_barrier_semaphore()
        def greet(k, _):
            pl.semaphore_signal(barrier, inc=1, device_id={'dap': (me + k) % n_dev}, device_id_type=MESH)
            return 0
        lax.fori_loop(1, n_dev, greet, 0)
        def first(b, _):
            row = lax.broadcasted_iota(jnp.int32, (N, QB), 0)
            lane = lax.broadcasted_iota(jnp.int32, (N, QB), 1)
            r = lane // R
            turn = (row == _index(*_place(b, r))*R + lane % R).astype(F32).astype(BF16)
            qs = pl.ds(pl.multiple_of(b*QB, QB), QB)
            for i in range(R):
                zb = jnp.dot(z_ref[i], turn, preferred_element_type=F32)
                z_s[i, :, qs] = zb.astype(BF16)
                y_s[i*C:(i+1)*C] = _ln_t(zb, col(0, 0), col(0, 1))
            put_bias(0, b, bias_rows(0, y_s[...]))
            return 0
        lax.fori_loop(0, BLOCKS, first, 0)
        pl.semaphore_wait(barrier, n_dev - 1)
        def gather(k):
            def each(b, _):
                stage(k, 0, b)
                return 0
            lax.fori_loop(0, BLOCKS, each, 0)
        gather(0)
        gather(1)
        prep_all()
        gather(2)
        gather(3)
        gather(4)
        lax.fori_loop(0, H, turn_bias, 0)
        to_f32_all(0)

    @pl.when((jb == 0) & (ps > 0))
    def _():
        stage(4, par, 0)
        to_f32_all(0)
        arrived(par)
        prep_all()
        slot(4, ps-1)

    @pl.when(jb > 0)
    def _():
        to_f32_all(jb)

    zl = jnp.zeros((KC, 256-2*C), BF16)
    zp = jnp.zeros((KC, QB), BF16)
    zv = jnp.zeros((D, 256-KC), BF16)
    zq = jnp.zeros((2*D, QB), BF16)
    steps = [(h, c) for h in range(H) for c in range(CH)]
    S = len(steps)
    es, ss, acc, tot = {}, {}, [None]*R, [None]*R
    for n in range(-LAG, S):
        if n >= 0:
            h, c = steps[n]
            b = bias_s[h, c*KC:(c+1)*KC]
            for i in range(R):
                e = jnp.exp2(ss.pop((n, i)) + b)
                es[i] = e.astype(BF16)
                e = jnp.sum(e.reshape(KC//8, 8, QB), axis=0)
                tot[i] = e if c == 0 else tot[i] + e
        for i in range(R):
            rows = []
            w = zp
            if n+LAG < S:
                h2, c2 = steps[n+LAG]
                w = jnp.concatenate([zq]*h2 + [q_s[i, 2*D*h2:2*D*(h2+1), pl.ds(q0, QB)]] + [zq]*(H-1-h2), axis=0)
                rows.append(jnp.concatenate([zl, k_s[i, c2*KC:(c2+1)*KC]], axis=1))
            if n >= 0:
                rows.append(jnp.concatenate([v_s[i, D*h:D*h+D, c*KC:(c+1)*KC], zv], axis=1))
            o = jnp.dot(jnp.concatenate(rows, axis=0), jnp.concatenate([es.pop(i) if n >= 0 else zp, w], axis=0),
                        preferred_element_type=F32)
            if n+LAG < S:
                ss[n+LAG, i] = o[0:KC]
            if n >= 0:
                o = o[-D:]
                acc[i] = o if c == 0 else acc[i] + o
                if c == CH-1:
                    a = acc[i] / jnp.sum(tot[i], axis=0, keepdims=True)
                    o_s[i, D*h:D*h+D] = (g_s[i, D*h:D*h+D, pl.ds(q0, QB)] * a).astype(BF16)

    for i in range(R):
        u = jnp.dot(wo_ref[ps], o_s[i], preferred_element_type=F32) + col(ps, 3)
        zt_s[i*C:(i+1)*C] = (z_s[i, :, pl.ds(q0, QB)].astype(F32) + u).astype(BF16)
    x_s[pl.ds(jb*DB, DB)] = zt_s[...].T.reshape(DB, R, R*C)

    def send(t, _):
        for j in range(4):
            k = 4*t + j
            d = _index(*_place(jb, k))
            @pl.when(d != me)
            def _():
                pltpu.make_async_remote_copy(x_s.at[jb*DB + k], r_s.at[nxt, slot_of_me], a2a_send, a2a_recv.at[nxt],
                                             device_id={'dap': d}, device_id_type=MESH).start()
        return 0
    lax.fori_loop(0, DB//4, send, 0)

    @pl.when(my_block == jb)
    def _():
        r_s[nxt, slot_of_me] = x_s[jb*DB + my_place]

    pn = (ps + 1) % n_pass
    for i in range(R):
        y_s[i*C:(i+1)*C] = _ln_t(zt_s[i*C:(i+1)*C].astype(F32), col(pn, 0), col(pn, 1))

    @pl.when(ps < n_pass-1)
    def _():
        put_bias(nxt, jb, bias_rows(pn, y_s[...]))
    slot(jb, ps)

    @pl.when((ps == n_pass-1) & (jb == BLOCKS-1))
    def _():
        arrived(nxt)
        out = pltpu.make_async_copy(z_s, out_ref, own_sem)
        out.start()
        out.wait()


def mega(z, mask, cols, wqvt, wk2, wo, wbn, LAG=2):
    R, C, N = z.shape
    n_pass = cols.shape[0]
    H = wbn.shape[1] // R
    QB = N // BLOCKS
    full = lambda a: pl.BlockSpec(a.shape, lambda p, j: (0,)*a.ndim, pipeline_mode=pl.Buffered(1))
    args = (z, mask, cols, wqvt, wk2, wo, wbn)
    dma = pltpu.SemaphoreType.DMA
    return pl.pallas_call(
        functools.partial(mega_kernel, R, N, C, H, LAG),
        grid=(n_pass, BLOCKS),
        in_specs=[full(a) for a in args],
        out_specs=pl.BlockSpec(memory_space=pl.ANY),
        out_shape=jax.ShapeDtypeStruct((R, C, N), BF16),
        scratch_shapes=[pltpu.VMEM((R, N, 2*C), BF16), pltpu.VMEM((R, 2*C, N), BF16), pltpu.VMEM((R, C, N), BF16),
                        pltpu.VMEM((R, C, N), F32), pltpu.VMEM((R, C, N), BF16), pltpu.VMEM((R, C, QB), BF16),
                        pltpu.VMEM((R*C, QB), BF16), pltpu.VMEM((R*C, QB), BF16), pltpu.VMEM((H, N, QB), F32),
                        pltpu.VMEM((N//R, R, R*C), BF16), pltpu.VMEM((2, N//R, R, R*C), BF16),
                        pltpu.VMEM((2, BLOCKS, T, T, T, 2, 2*H, R, 128), BF16),
                        dma, dma((2,)), dma, dma((2, BLOCKS, 5)), dma((2, BLOCKS, 5))],
        compiler_params=pltpu.CompilerParams(dimension_semantics=("arbitrary", "arbitrary"), vmem_limit_bytes=60*2**20,
                                             collective_id=0, has_side_effects=True),
        cost_estimate=pl.CostEstimate(flops=n_pass*4*R*H*N*N*(C//H), bytes_accessed=4*N*R*C, transcendentals=n_pass*R*H*N*N),
        name="mega",
    )(*args)


def _ln_rows(x, w):
    x = x.astype(F32)
    mu = jnp.mean(x, axis=-1, keepdims=True)
    var = jnp.mean(jnp.square(x - mu), axis=-1, keepdims=True)
    y = (x - mu) * lax.rsqrt(var + EPS)
    return (y * w[0].astype(F32) + w[1].astype(F32)).astype(BF16)


def _rows(zl, bias, lw, wi, bg, wo, bo):
    h, n, _ = bias.shape
    c = zl.shape[-1]
    d = c // h

    def row(zr):
        y = _ln_rows(zr, lw)
        proj = jnp.transpose(jnp.dot(y, wi, preferred_element_type=F32).reshape(n, 4, h, d), (1, 2, 0, 3))
        gate = jax.nn.sigmoid(proj[3] + bg.astype(F32).reshape(h, 1, d))

        def head(a):
            q, k, v, b = a
            s = jnp.dot(q, k.T, preferred_element_type=F32) * d ** -0.5 + b
            return jnp.dot(jax.nn.softmax(s, axis=-1).astype(BF16), v, preferred_element_type=F32)

        o = lax.map(head, (*(a.astype(BF16) for a in proj[:3]), bias))
        o = jnp.transpose((gate * o).astype(BF16), (1, 0, 2)).reshape(n, c)
        return (zr.astype(F32) + jnp.dot(o, wo, preferred_element_type=F32) + bo.astype(F32)).astype(BF16)

    return lax.map(row, zl)


def solution(mesh):
    def local(zl, res_mask, ln_w, w_in, b_g, w_b, w_o, b_o):
        R, N, C = zl.shape
        n = ln_w.shape[0] * ln_w.shape[1]
        ws = tuple(a.reshape(n, *a.shape[2:]) for a in (ln_w, w_in, b_g, w_b, w_o, b_o))
        cols, wqvt, wk2, wo, wbn, mask, ok = setup(ws, res_mask, R)

        def fast(zl):
            return jnp.swapaxes(mega(jnp.swapaxes(zl, 1, 2), mask, cols, wqvt, wk2, wo, wbn), 1, 2)

        def exact(zl):
            mask_bias = jnp.where(res_mask > 0, 0.0, NEG).astype(F32)

            def one(p, z):
                lw, wi, bg, wb, wo, bo = (lax.dynamic_index_in_dim(a, p, keepdims=False) for a in ws)
                b = jnp.dot(_ln_rows(z, lw).reshape(R*N, C), wb, preferred_element_type=F32).astype(BF16)
                b = jnp.transpose(b.reshape(R, 8, N//8, -1), (3, 1, 0, 2))
                b = b.reshape(-1, R, N//8)
                bias = lax.map(lambda a: lax.all_gather(a, 'dap', axis=0, tiled=True), b)
                bias = jnp.swapaxes(bias.reshape(-1, 8, N, N//8), 1, 2).reshape(-1, N, N)
                z = _rows(z, bias.astype(F32) + mask_bias, lw, wi, bg, wo, bo)
                return jnp.swapaxes(lax.all_to_all(z, 'dap', 1, 0, tiled=True), 0, 1)
            return lax.fori_loop(0, n, one, zl)

        return lax.cond(ok[0, 0] > 0, fast, exact, zl)

    rows = P(('data', 'dap'))
    return jax.shard_map(local, mesh=mesh,
                         in_specs=(rows, P('data'), P(), P(), P(), P(), P(), P()),
                         out_specs=rows, check_vma=False)
```
